512 devices in a mesh: sub: 8 (over y), row: 8 (over x, core), col: 8 (over z).
Axes of the slice: x: 4, y: 8, z: 8, core: 2. Of those that a mesh axis runs over, the one named last changes fastest.
Arguments:
- visibility: bfloat16 [2, 64, 512, 4096], P(None, 'sub', 'row', 'col'), may hold values from -13 to 13
- sky_model: bfloat16 [2, 64, 512, 4096], P(None, 'sub', 'row', 'col'), may hold values from -4 to 4, as said below
- antenna_flags: int32 [8, 512], P('sub'), may hold values 0 or 1
- gains_init: float32 [2, 64, 512], P(None, 'sub'), may hold values from -0.5 to 1.5
Outputs:
- gains: float32 [2, 64, 512], P(None, 'sub')
The draws below stay inside these ranges and needn't reach their ends.
Inputs may be any that keep to these rules, and one draw needn't show every extreme that they name: `sky_model`: model visibility parts lie between -4 and 4.
All inputs are finite; a program needn't handle non-finite values.
Results may differ from the reference program's by a relative error of at most 0.0003.
Values sent between devices are 32-bit elements.
No kernel may reach another device: no remote copies, remote signals or barrier semaphores. Data moves between devices by JAX's collectives and lax.ppermute only.
A program may use at most 64 MiB of HBM per device.

```python
import jax
import jax.numpy as jnp
from jax import lax

ANTENNAS = 512
CH_SUB = 8
TIMES = 8
ITERS = 3
SUBBANDS = 8
CHANNELS = 64
N_SUB = 8


def sky_draw(key):
    full_shape = (CHANNELS, ANTENNAS, ANTENNAS, TIMES)
    model_re = jnp.clip(jax.random.normal(jax.random.fold_in(key, 11), full_shape, jnp.float32), -4.0, 4.0)
    model_im = jnp.clip(jax.random.normal(jax.random.fold_in(key, 21), full_shape, jnp.float32), -4.0, 4.0)
    base_re = jax.random.uniform(jax.random.fold_in(key, 12), (SUBBANDS, 1, ANTENNAS), jnp.float32, 0.6, 1.3)
    base_im = jax.random.uniform(jax.random.fold_in(key, 22), (SUBBANDS, 1, ANTENNAS), jnp.float32, -0.3, 0.3)
    wiggle = jax.random.uniform(jax.random.fold_in(key, 13), (SUBBANDS, CH_SUB, ANTENNAS), jnp.float32, -0.1, 0.1)
    gain_re = (base_re + wiggle).reshape(CHANNELS, ANTENNAS)
    gain_im = jnp.broadcast_to(base_im, (SUBBANDS, CH_SUB, ANTENNAS)).reshape(CHANNELS, ANTENNAS)
    pair_re = gain_re[:, :, None, None] * gain_re[:, None, :, None] + gain_im[:, :, None, None] * gain_im[:, None, :, None]
    pair_im = gain_im[:, :, None, None] * gain_re[:, None, :, None] - gain_re[:, :, None, None] * gain_im[:, None, :, None]
    noise_re = 0.2 * jnp.clip(jax.random.normal(jax.random.fold_in(key, 14), full_shape, jnp.float32), -4.0, 4.0)
    noise_im = 0.2 * jnp.clip(jax.random.normal(jax.random.fold_in(key, 24), full_shape, jnp.float32), -4.0, 4.0)
    observed_re = pair_re * model_re - pair_im * model_im + noise_re
    observed_im = pair_re * model_im + pair_im * model_re + noise_im
    flat_shape = (CHANNELS, ANTENNAS, ANTENNAS * TIMES)
    model_both = jnp.stack([model_re.reshape(flat_shape), model_im.reshape(flat_shape)], axis=0)
    observed_both = jnp.stack([observed_re.reshape(flat_shape), observed_im.reshape(flat_shape)], axis=0)
    return (model_both, observed_both)


def draw_visibility(key, part):
    return sky_draw(key)[1].astype(jnp.bfloat16)


def draw_sky_model(key, part):
    return sky_draw(key)[0].astype(jnp.bfloat16)


def plant(entries, key, low, high):
    index_at = [jax.random.randint(jax.random.fold_in(key, axis), (), 0, length) for axis, length in enumerate(entries.shape)]
    main_axis = entries.shape.index(max(entries.shape))
    neighbour = index_at[:main_axis] + [(index_at[main_axis] + 1) % entries.shape[main_axis]] + index_at[main_axis + 1:]
    return entries.at[tuple(index_at)].set(low).at[tuple(neighbour)].set(high)


def block_scale(own_key, extent, shards, smallest, top_value):
    level, own = 1.0, jax.random.fold_in(own_key, 6)
    for dim, shards_of in shards:
        draws = jnp.exp(jax.random.uniform(jax.random.fold_in(own, dim), (shards_of,), jnp.float32, smallest / len(shards), top_value / len(shards)))
        level = level * jnp.repeat(draws, extent[dim] // shards_of).reshape([-1 if axis == dim else 1 for axis in range(len(extent))])
    return level


def setup_inputs(seed: int = 0) -> dict:
    splits = jax.random.split(jax.random.key(seed), 5)
    return {
        "visibility": draw_visibility(jax.random.fold_in(splits[4], 71), 0),
        "sky_model": draw_sky_model(jax.random.fold_in(splits[4], 71), 0),
        "antenna_flags": plant((jax.random.randint(splits[2], (SUBBANDS, ANTENNAS), 0, 8) < 7).astype(jnp.int32), jax.random.fold_in(splits[2], 1), 0, 1),
        "gains_init": jnp.clip(-0.5 + 2.0 * jax.random.uniform(splits[3], (2, CHANNELS, ANTENNAS), jnp.float32) ** block_scale(splits[3], (2, CHANNELS, ANTENNAS), ((1, 8),), -0.2, 0.2), -0.5, 1.5),
    }


def reference(visibility, sky_model, antenna_flags, gains_init):
    flag_values = antenna_flags.astype(jnp.float32)
    chan_flags = jnp.repeat(flag_values, CH_SUB, axis=0)
    off_diagonal = jnp.float32(1.0) - jnp.eye(ANTENNAS, dtype=jnp.float32)

    def prepare(bundle):
        vis_real, vis_imag, model_real, model_imag, flag_slice = bundle
        shape_three = (ANTENNAS, ANTENNAS, TIMES)
        vis_re = vis_real.astype(jnp.float32).reshape(shape_three)
        vis_im = vis_imag.astype(jnp.float32).reshape(shape_three)
        mod_re = model_real.astype(jnp.float32).reshape(shape_three)
        mod_im = model_imag.astype(jnp.float32).reshape(shape_three)
        weight = flag_slice[:, None] * flag_slice[None, :] * off_diagonal
        cross_re = jnp.sum(vis_re * mod_re + vis_im * mod_im, axis=2) * weight
        cross_im = jnp.sum(vis_im * mod_re - vis_re * mod_im, axis=2) * weight
        power_sum = jnp.sum(mod_re * mod_re + mod_im * mod_im, axis=2) * weight
        return cross_re, cross_im, power_sum

    cross_re, cross_im, power_sum = lax.map(prepare, (visibility[0], visibility[1], sky_model[0], sky_model[1], chan_flags))

    def contract(matrix, vector):
        return jnp.einsum("cpq,cq->cp", matrix, vector, precision=lax.Precision.HIGHEST)

    gain_values = gains_init
    for step_index in range(ITERS):
        gain_re = gain_values[0]
        gain_im = gain_values[1]
        num_re = contract(cross_re, gain_re) - contract(cross_im, gain_im)
        num_im = contract(cross_re, gain_im) + contract(cross_im, gain_re)
        denominator = contract(power_sum, gain_re * gain_re + gain_im * gain_im) + 1.0
        quotient = jnp.stack([num_re / denominator, num_im / denominator], axis=0)
        updated = 0.5 * (quotient + gain_values)
        grouped = updated.reshape(2, N_SUB, CH_SUB, ANTENNAS)
        chan_mean = jnp.mean(grouped, axis=2)
        overall = jnp.mean(chan_mean, axis=1)
        gain_values = (grouped + 0.5 * (overall[:, None, None, :] - chan_mean[:, :, None, :])).reshape(2, CHANNELS, ANTENNAS)
    return gain_values
```

```python
import jax
import jax.numpy as jnp
from jax import lax
from jax.experimental import pallas as pl
from jax.experimental.pallas import tpu as pltpu
from jax.sharding import PartitionSpec as P


TIMES = 8
PEERS = 8
HALF = 64
F32 = jnp.float32
VMEM = pl.BlockSpec(memory_space=pltpu.VMEM)


def low_lanes(rows):
    return lax.broadcasted_iota(jnp.int32, (rows, 128), 1) < HALF


def swap(value):
    return pltpu.roll(value, HALF, 1)


def own_half(slab, odd):
    return jnp.where(odd, swap(slab), slab)


def spread(gains):
    turned = gains.T
    low = low_lanes(HALF)
    columns = []
    for row in range(8):
        first = jnp.broadcast_to(turned[:HALF, row : row + 1], (HALF, 128))
        second = jnp.broadcast_to(turned[HALF:, row : row + 1], (HALF, 128))
        columns.append(jnp.where(low, first, second))
    return columns[:4], columns[4:]


def products(cross_re, cross_im, power, gain_re, gain_im):
    over = lambda value: jnp.sum(value, axis=0, keepdims=True)
    return (
        over(cross_re * gain_re - cross_im * gain_im),
        over(cross_re * gain_im + cross_im * gain_re),
        over(power * (gain_re * gain_re + gain_im * gain_im)),
    )


def contract(tile, gains, sums):
    gain_re, gain_im = spread(gains)
    for j in range(4):
        rows = products(tile[0, j], tile[1, j], tile[2, j], gain_re[j], gain_im[j])
        for part in range(3):
            sums[part * 4 + j : part * 4 + j + 1, :] = rows[part]


def first_kernel(vis, sky, flags, init, tile, message, weight, gain, selector, sums):
    j = pl.program_id(0)
    row = lax.axis_index("row")
    col = lax.axis_index("col")

    @pl.when(j == 0)
    def _():
        low = low_lanes(4)

        def block(ref, index, lead):
            start = pl.multiple_of(lax.shift_right_logical(index, 1) * 128, 128)
            return own_half(ref[lead + (slice(None), pl.ds(start, 128))], lax.rem(index, 2) == 1)

        packed = []
        for part in range(2):
            mine = block(init, col, (part,))
            packed.append(jnp.where(low, mine[:4], swap(mine)[4:]))
        gain_re, gain_im = spread(jnp.concatenate(packed, axis=0))
        for k in range(4):
            gain[0, k] = gain_re[k]
            gain[1, k] = gain_im[k]
        row_flag = block(flags, row, ()).astype(F32)
        row_flag = jnp.where(low_lanes(1), row_flag, swap(row_flag))
        col_flag = jnp.broadcast_to(block(flags, col, ()).astype(F32), (8, 128)).T[:HALF, 0:1]
        col_ids = col * HALF + lax.broadcasted_iota(jnp.int32, (HALF, 128), 0)
        row_ids = row * HALF + (lax.broadcasted_iota(jnp.int32, (HALF, 128), 1) & (HALF - 1))
        weight[...] = jnp.where(col_ids != row_ids, col_flag * row_flag, 0.0)
        wide = lax.broadcasted_iota(jnp.int32, (HALF, HALF * TIMES), 1)
        narrow = lax.broadcasted_iota(jnp.int32, (HALF, HALF * TIMES), 0)
        selector[...] = jnp.where(lax.shift_right_logical(wide, 3) == narrow, 1.0, 0.0).astype(jnp.bfloat16)

    def wide_part(ref, part):
        return ref[part, :, 0].reshape(128, HALF * TIMES).astype(F32)

    vis_re, vis_im = wide_part(vis, 0), wide_part(vis, 1)
    mod_re, mod_im = wide_part(sky, 0), wide_part(sky, 1)
    chosen = selector[...]

    def time_total(value):
        high = value.astype(jnp.bfloat16)
        rest = (value - high.astype(F32)).astype(jnp.bfloat16)
        dims = (((1,), (1,)), ((), ()))
        total = lax.dot_general(chosen, high, dims, preferred_element_type=F32)
        return total + lax.dot_general(chosen, rest, dims, preferred_element_type=F32)

    scale = weight[...]
    cross_re = time_total(vis_re * mod_re + vis_im * mod_im) * scale
    cross_im = time_total(vis_im * mod_re - vis_re * mod_im) * scale
    power = time_total(mod_re * mod_re + mod_im * mod_im) * scale
    tile[0, 0] = cross_re
    tile[1, 0] = cross_im
    tile[2, 0] = power
    rows = products(cross_re, cross_im, power, gain[0, j], gain[1, j])
    for part in range(3):
        sums[pl.ds(part * 4 + j, 1), :] = rows[part]

    @pl.when(j == 3)
    def _():
        for peer in range(PEERS):
            message[peer] = sums[...]


def update(summed, previous, mean, rest):
    denominator = summed[8:12] + 1.0
    updated = 0.5 * (jnp.concatenate([summed[0:4] / denominator, summed[4:8] / denominator], axis=0) + previous)
    means = []
    kept = []
    for part in range(2):
        values = updated[part * 4 : part * 4 + 4]
        total = jnp.sum(values, axis=0, keepdims=True)
        total = (total + swap(total)) / 8.0
        means.append(total)
        kept.append(values - 0.5 * total)
    mean[...] = jnp.broadcast_to(jnp.where(low_lanes(1), means[0], means[1]), (PEERS, 128))
    rest[...] = jnp.concatenate(kept, axis=0)


def first_update_kernel(received, init, mean, rest):
    row = lax.axis_index("row")
    start = pl.multiple_of(lax.shift_right_logical(row, 1) * 128, 128)
    low = low_lanes(4)
    packed = []
    for part in range(2):
        mine = own_half(init[part, :, pl.ds(start, 128)], lax.rem(row, 2) == 1)
        packed.append(jnp.where(low, mine[:4], swap(mine)[4:]))
    update(jnp.sum(received[...], axis=0), jnp.concatenate(packed, axis=0), mean, rest)


def update_kernel(owner, received, mean, rest):
    previous = received[lax.axis_index(owner), 12:20]
    update(jnp.sum(received[:, 0:12], axis=0), previous, mean, rest)


def add_overall(means, rest):
    overall = jnp.sum(means[...], axis=0, keepdims=True) / 16.0
    other = swap(overall)
    low = low_lanes(1)
    return jnp.concatenate(
        [rest[0:4] + jnp.where(low, overall, other), rest[4:8] + jnp.where(low, other, overall)], axis=0
    )


def contract_kernel(means, rest, tile, message, sums):
    gains = add_overall(means, rest)
    contract(tile, gains, sums)
    sums[12:20, :] = gains
    sums[20:24, :] = jnp.zeros((4, 128), F32)
    for peer in range(PEERS):
        message[peer] = sums[...]


def share_kernel(means, rest, message):
    gains = add_overall(means, rest)
    for peer in range(PEERS):
        message[peer] = gains


def collect_kernel(received, out):
    low = low_lanes(4)
    for part in range(2):
        for pair in range(4):
            even = received[2 * pair, part * 4 : part * 4 + 4]
            odd = received[2 * pair + 1, part * 4 : part * 4 + 4]
            out[part, 0:4, pair * 128 : pair * 128 + 128] = jnp.where(low, even, swap(odd))
            out[part, 4:8, pair * 128 : pair * 128 + 128] = jnp.where(low, swap(even), odd)


def shaped(*shape):
    return jax.ShapeDtypeStruct(shape, F32)


def call(kernel, outs, *args, scratch=()):
    return pl.pallas_call(
        kernel,
        out_shape=outs,
        in_specs=[VMEM] * len(args),
        out_specs=jax.tree.map(lambda _: VMEM, outs),
        scratch_shapes=scratch,
        compiler_params=pltpu.CompilerParams(vmem_limit_bytes=4 << 20),
        name=kernel.__name__,
    )(*args)


def exchange(message, axis):
    return lax.all_to_all(message, axis, 0, 0, tiled=True)


def body(visibility, sky_model, antenna_flags, gains_init):
    wide = (2, 2, 4, HALF, HALF * TIMES)
    whole = lambda shape: pl.BlockSpec(shape, lambda j: (0,) * len(shape))
    data = pl.BlockSpec((2, 2, 1, HALF, HALF * TIMES), lambda j: (0, 0, j, 0, 0))
    tile, message = pl.pallas_call(
        first_kernel,
        grid=(4,),
        out_shape=(shaped(3, 4, HALF, 128), shaped(PEERS, 12, 128)),
        in_specs=[data, data, whole((1, 512)), whole((2, 8, 512))],
        out_specs=(pl.BlockSpec((3, 1, HALF, 128), lambda j: (0, j, 0, 0)), whole((PEERS, 12, 128))),
        scratch_shapes=[
            pltpu.VMEM((HALF, 128), F32),
            pltpu.VMEM((2, 4, HALF, 128), F32),
            pltpu.VMEM((HALF, HALF * TIMES), jnp.bfloat16),
            pltpu.VMEM((12, 128), F32),
        ],
        compiler_params=pltpu.CompilerParams(vmem_limit_bytes=12 << 20),
        name="first_kernel",
    )(visibility.reshape(wide), sky_model.reshape(wide), antenna_flags, gains_init)
    outs = (shaped(PEERS, 128), shaped(8, 128))
    sums = [pltpu.VMEM((24, 128), F32)]

    received = exchange(message, "col")
    mean, rest = call(first_update_kernel, outs, received, gains_init)
    tile, mean = lax.optimization_barrier((tile, mean))
    turned = lax.ppermute(
        tile, ("row", "col"), [(r * 8 + c, c * 8 + r) for r in range(8) for c in range(8)]
    )
    means = exchange(mean, "sub")
    message = call(contract_kernel, shaped(PEERS, 24, 128), means, rest, turned, scratch=sums)
    received = exchange(message, "row")

    def after_row(received, mean, rest):
        update_kernel("col", received, mean, rest)

    def after_col(received, mean, rest):
        update_kernel("row", received, mean, rest)

    mean, rest = call(after_row, outs, received)
    means = exchange(mean, "sub")
    message = call(contract_kernel, shaped(PEERS, 24, 128), means, rest, tile, scratch=sums)
    received = exchange(message, "col")
    mean, rest = call(after_col, outs, received)
    means = exchange(mean, "sub")
    message = call(share_kernel, shaped(PEERS, 8, 128), means, rest)
    received = exchange(message, "row")
    return call(collect_kernel, shaped(2, 8, 512), received)


def solution(mesh):
    return jax.shard_map(
        body,
        mesh=mesh,
        in_specs=(
            P(None, "sub", "row", "col"),
            P(None, "sub", "row", "col"),
            P("sub", None),
            P(None, "sub", None),
        ),
        out_specs=P(None, "sub", None),
        check_vma=False,
    )
```

```python
import jax
import jax.numpy as jnp
from jax import lax
from jax.experimental import pallas as pl
from jax.experimental.pallas import tpu as pltpu
from jax.sharding import PartitionSpec as P


TIMES = 8
PEERS = 8
HALF = 64
F32 = jnp.float32
FIRST_LIMIT = 16 << 20
VMEM = pl.BlockSpec(memory_space=pltpu.VMEM)


def low_lanes(rows):
    return lax.broadcasted_iota(jnp.int32, (rows, 128), 1) < HALF


def swap(value):
    return pltpu.roll(value, HALF, 1)


def own_half(slab, odd):
    return jnp.where(odd, swap(slab), slab)


def spread(gains):
    turned = gains.T
    low = low_lanes(HALF)
    columns = []
    for row in range(8):
        first = jnp.broadcast_to(turned[:HALF, row : row + 1], (HALF, 128))
        second = jnp.broadcast_to(turned[HALF:, row : row + 1], (HALF, 128))
        columns.append(jnp.where(low, first, second))
    return columns[:4], columns[4:]


def products(cross_re, cross_im, power, gain_re, gain_im):
    over = lambda value: jnp.sum(value, axis=0, keepdims=True)
    return (
        over(cross_re * gain_re - cross_im * gain_im),
        over(cross_re * gain_im + cross_im * gain_re),
        over(power * (gain_re * gain_re + gain_im * gain_im)),
    )


def contract(tile, gains, sums):
    gain_re, gain_im = spread(gains)
    for j in range(4):
        rows = products(tile[0, j], tile[1, j], tile[2, j], gain_re[j], gain_im[j])
        for part in range(3):
            sums[part * 4 + j : part * 4 + j + 1, :] = rows[part]


def first_kernel(vis_hbm, sky_hbm, flags_hbm, init_hbm, tile, message, vis, sky, flags, init, sums, small_sems, wide_sems):
    row = lax.axis_index("row")
    col = lax.axis_index("col")
    small = [
        pltpu.make_async_copy(flags_hbm, flags, small_sems.at[0]),
        pltpu.make_async_copy(init_hbm, init, small_sems.at[1]),
    ]
    wide = [
        [
            pltpu.make_async_copy(source.at[:, :, j], target.at[j], wide_sems.at[which, j])
            for which, (source, target) in enumerate(((vis_hbm, vis), (sky_hbm, sky)))
        ]
        for j in range(4)
    ]
    for copy in small + sum(wide, []):
        copy.start()

    long = lax.broadcasted_iota(jnp.int32, (HALF, HALF * TIMES), 1)
    short = lax.broadcasted_iota(jnp.int32, (HALF, HALF * TIMES), 0)
    chosen = jnp.where(lax.shift_right_logical(long, 3) == short, 1.0, 0.0).astype(jnp.bfloat16)
    for copy in small:
        copy.wait()
    low = low_lanes(4)

    def block(ref, index, lead):
        start = pl.multiple_of(lax.shift_right_logical(index, 1) * 128, 128)
        return own_half(ref[lead + (slice(None), pl.ds(start, 128))], lax.rem(index, 2) == 1)

    packed = []
    for part in range(2):
        mine = block(init, col, (part,))
        packed.append(jnp.where(low, mine[:4], swap(mine)[4:]))
    gain_re, gain_im = spread(jnp.concatenate(packed, axis=0))
    row_flag = block(flags, row, ()).astype(F32)
    row_flag = jnp.where(low_lanes(1), row_flag, swap(row_flag))
    col_flag = jnp.broadcast_to(block(flags, col, ()).astype(F32), (8, 128)).T[:HALF, 0:1]
    col_ids = col * HALF + lax.broadcasted_iota(jnp.int32, (HALF, 128), 0)
    row_ids = row * HALF + (lax.broadcasted_iota(jnp.int32, (HALF, 128), 1) & (HALF - 1))
    scale = jnp.where(col_ids != row_ids, col_flag * row_flag, 0.0)

    def time_total(value):
        high = value.astype(jnp.bfloat16)
        rest = (value - high.astype(F32)).astype(jnp.bfloat16)
        dims = (((1,), (1,)), ((), ()))
        total = lax.dot_general(chosen, high, dims, preferred_element_type=F32)
        return total + lax.dot_general(chosen, rest, dims, preferred_element_type=F32)

    for j in range(4):
        for copy in wide[j]:
            copy.wait()

        def wide_part(ref, part):
            return ref[j, part].reshape(128, HALF * TIMES).astype(F32)

        vis_re, vis_im = wide_part(vis, 0), wide_part(vis, 1)
        mod_re, mod_im = wide_part(sky, 0), wide_part(sky, 1)
        cross_re = time_total(vis_re * mod_re + vis_im * mod_im) * scale
        cross_im = time_total(vis_im * mod_re - vis_re * mod_im) * scale
        power = time_total(mod_re * mod_re + mod_im * mod_im) * scale
        tile[0, j] = cross_re
        tile[1, j] = cross_im
        tile[2, j] = power
        rows = products(cross_re, cross_im, power, gain_re[j], gain_im[j])
        for part in range(3):
            sums[part * 4 + j : part * 4 + j + 1, :] = rows[part]
    for peer in range(PEERS):
        message[peer] = sums[...]


def update(summed, previous, mean, rest):
    denominator = summed[8:12] + 1.0
    updated = 0.5 * (jnp.concatenate([summed[0:4] / denominator, summed[4:8] / denominator], axis=0) + previous)
    means = []
    kept = []
    for part in range(2):
        values = updated[part * 4 : part * 4 + 4]
        total = jnp.sum(values, axis=0, keepdims=True)
        total = (total + swap(total)) / 8.0
        means.append(total)
        kept.append(values - 0.5 * total)
    mean[...] = jnp.broadcast_to(jnp.where(low_lanes(1), means[0], means[1]), (PEERS, 128))
    rest[...] = jnp.concatenate(kept, axis=0)


def first_update_kernel(received, init, mean, rest):
    row = lax.axis_index("row")
    start = pl.multiple_of(lax.shift_right_logical(row, 1) * 128, 128)
    low = low_lanes(4)
    packed = []
    for part in range(2):
        mine = own_half(init[part, :, pl.ds(start, 128)], lax.rem(row, 2) == 1)
        packed.append(jnp.where(low, mine[:4], swap(mine)[4:]))
    update(jnp.sum(received[...], axis=0), jnp.concatenate(packed, axis=0), mean, rest)


def update_kernel(owner, received, mean, rest):
    previous = received[lax.axis_index(owner), 12:20]
    update(jnp.sum(received[:, 0:12], axis=0), previous, mean, rest)


def add_overall(means, rest):
    overall = jnp.sum(means[...], axis=0, keepdims=True) / 16.0
    other = swap(overall)
    low = low_lanes(1)
    return jnp.concatenate(
        [rest[0:4] + jnp.where(low, overall, other), rest[4:8] + jnp.where(low, other, overall)], axis=0
    )


def contract_kernel(means, rest, tile, message, sums):
    gains = add_overall(means, rest)
    contract(tile, gains, sums)
    sums[12:20, :] = gains
    sums[20:24, :] = jnp.zeros((4, 128), F32)
    for peer in range(PEERS):
        message[peer] = sums[...]


def share_kernel(means, rest, message):
    gains = add_overall(means, rest)
    for peer in range(PEERS):
        message[peer] = gains


def collect_kernel(received, out):
    low = low_lanes(4)
    for part in range(2):
        for pair in range(4):
            even = received[2 * pair, part * 4 : part * 4 + 4]
            odd = received[2 * pair + 1, part * 4 : part * 4 + 4]
            out[part, 0:4, pair * 128 : pair * 128 + 128] = jnp.where(low, even, swap(odd))
            out[part, 4:8, pair * 128 : pair * 128 + 128] = jnp.where(low, swap(even), odd)


def shaped(*shape):
    return jax.ShapeDtypeStruct(shape, F32)


def call(kernel, outs, *args, scratch=()):
    return pl.pallas_call(
        kernel,
        out_shape=outs,
        in_specs=[VMEM] * len(args),
        out_specs=jax.tree.map(lambda _: VMEM, outs),
        scratch_shapes=scratch,
        compiler_params=pltpu.CompilerParams(vmem_limit_bytes=4 << 20),
        name=kernel.__name__,
    )(*args)


def exchange(message, axis):
    return lax.all_to_all(message, axis, 0, 0, tiled=True)


def body(visibility, sky_model, antenna_flags, gains_init):
    wide = (2, 2, 4, HALF, HALF * TIMES)
    stay = pl.BlockSpec(memory_space=pl.ANY)
    tile, message = pl.pallas_call(
        first_kernel,
        out_shape=(shaped(3, 4, HALF, 128), shaped(PEERS, 12, 128)),
        in_specs=[stay] * 4,
        out_specs=(VMEM, VMEM),
        scratch_shapes=[
            pltpu.VMEM((4, 2, 2, HALF, HALF * TIMES), jnp.bfloat16),
            pltpu.VMEM((4, 2, 2, HALF, HALF * TIMES), jnp.bfloat16),
            pltpu.VMEM((1, 512), jnp.int32),
            pltpu.VMEM((2, 8, 512), F32),
            pltpu.VMEM((12, 128), F32),
            pltpu.SemaphoreType.DMA((2,)),
            pltpu.SemaphoreType.DMA((2, 4)),
        ],
        compiler_params=pltpu.CompilerParams(vmem_limit_bytes=FIRST_LIMIT),
        name="first_kernel",
    )(*[pltpu.with_memory_space_constraint(x, pltpu.HBM) for x in (visibility.reshape(wide), sky_model.reshape(wide), antenna_flags, gains_init)])
    outs = (shaped(PEERS, 128), shaped(8, 128))
    sums = [pltpu.VMEM((24, 128), F32)]

    received = exchange(message, "col")
    mean, rest = call(first_update_kernel, outs, received, gains_init)
    turned = lax.ppermute(
        tile, ("row", "col"), [(r * 8 + c, c * 8 + r) for r in range(8) for c in range(8)]
    )
    means = exchange(mean, "sub")
    message = call(contract_kernel, shaped(PEERS, 24, 128), means, rest, turned, scratch=sums)
    received = exchange(message, "row")

    def after_row(received, mean, rest):
        update_kernel("col", received, mean, rest)

    def after_col(received, mean, rest):
        update_kernel("row", received, mean, rest)

    mean, rest = call(after_row, outs, received)
    means = exchange(mean, "sub")
    message = call(contract_kernel, shaped(PEERS, 24, 128), means, rest, tile, scratch=sums)
    received = exchange(message, "col")
    mean, rest = call(after_col, outs, received)
    means = exchange(mean, "sub")
    message = call(share_kernel, shaped(PEERS, 8, 128), means, rest)
    received = exchange(message, "row")
    return call(collect_kernel, shaped(2, 8, 512), received)


def solution(mesh):
    return jax.shard_map(
        body,
        mesh=mesh,
        in_specs=(
            P(None, "sub", "row", "col"),
            P(None, "sub", "row", "col"),
            P("sub", None),
            P(None, "sub", None),
        ),
        out_specs=P(None, "sub", None),
        check_vma=False,
    )
```

```python
import functools

import jax
import jax.numpy as jnp
from jax import lax
from jax.experimental import pallas as pl
from jax.experimental.pallas import tpu as pltpu
from jax.sharding import PartitionSpec as P


TIMES = 8
PEERS = 8
HALF = 64
F32 = jnp.float32
FIRST_LIMIT = 16 << 20
TILE_ROWS = 96
VMEM = pl.BlockSpec(memory_space=pltpu.VMEM)


def low_lanes(rows):
    return lax.broadcasted_iota(jnp.int32, (rows, 128), 1) < HALF


def swap(value):
    return pltpu.roll(value, HALF, 1)


def own_half(slab, odd):
    return jnp.where(odd, swap(slab), slab)


def spread(gains):
    turned = gains.T
    low = low_lanes(HALF)
    columns = []
    for row in range(8):
        first = jnp.broadcast_to(turned[:HALF, row : row + 1], (HALF, 128))
        second = jnp.broadcast_to(turned[HALF:, row : row + 1], (HALF, 128))
        columns.append(jnp.where(low, first, second))
    return columns[:4], columns[4:]


def products(cross_re, cross_im, power, gain_re, gain_im):
    over = lambda value: jnp.sum(value, axis=0, keepdims=True)
    return (
        over(cross_re * gain_re - cross_im * gain_im),
        over(cross_re * gain_im + cross_im * gain_re),
        over(power * (gain_re * gain_re + gain_im * gain_im)),
    )


def lanes_of(rows):
    return lax.broadcasted_iota(jnp.int32, (rows, 128), 1)


def slide(value, step):
    line = lax.broadcasted_iota(jnp.int32, (8, 128), 0)
    for bit in (1, 2, 4):
        value = jnp.where((line & bit) != 0, pltpu.roll(value, (step * bit) % 128, 1), value)
    return value


def pack(wide, which):
    lane = lanes_of(8)
    near = pltpu.roll(wide, (128 - 8 * which) % 128, 1)
    far = pltpu.roll(wide, (200 - 8 * which) % 128, 1)
    value = jnp.where(lane < 8, near, jnp.where(lane < 16, far, 0.0))
    return jnp.sum(slide(value, 16), axis=0, keepdims=True)


def pack_all(wide):
    return jnp.concatenate([pack(wide, which) for which in range(8)], axis=0)


def unpack(packed):
    group = lax.shift_right_logical(lanes_of(8), 3)
    wide = jnp.zeros((8, 128), F32)
    for which in range(8):
        line = jnp.broadcast_to(packed[which : which + 1], (8, 128))
        line = slide(line, -16)
        near = pltpu.roll(line, 8 * which, 1)
        far = pltpu.roll(line, (8 * which + 56) % 128, 1)
        wide = jnp.where(group == which, near, jnp.where(group == which + 8, far, wide))
    return wide


def channel_mean(packed):
    lane = lanes_of(8) & (HALF - 1)
    total = packed
    for step in (8, 16, 32):
        total = total + jnp.where(lane >= step, pltpu.roll(total, step, 1), pltpu.roll(total, step + HALF, 1))
    return total / 8.0


def smoothed(updated, sub):
    overall = jnp.sum(updated[...], axis=0) / 8.0
    own = updated[sub]
    return own + 0.5 * channel_mean(overall - own)


def spread_packed(gains):
    turned = gains.T
    low = low_lanes(8)
    columns = []
    for row in range(8):
        pieces = []
        for which in range(8):
            first = jnp.broadcast_to(turned[row * 16 : row * 16 + 8, which : which + 1], (8, 128))
            second = jnp.broadcast_to(turned[row * 16 + 8 : row * 16 + 16, which : which + 1], (8, 128))
            pieces.append(jnp.where(low, first, second))
        columns.append(pieces)
    return columns[:4], columns[4:]


def contract(tile, gains, sums):
    gain_re, gain_im = spread_packed(gains)
    for j in range(4):
        totals = [jnp.zeros((8, 128), F32)] * 3
        for which in range(8):
            cross_re, cross_im, power = [
                tile[which, (part * 4 + j) * 8 : (part * 4 + j) * 8 + 8] for part in range(3)
            ]
            re, im = gain_re[j][which], gain_im[j][which]
            totals[0] += cross_re * re - cross_im * im
            totals[1] += cross_re * im + cross_im * re
            totals[2] += power * (re * re + im * im)
        for part in range(3):
            sums[part * 4 + j : part * 4 + j + 1, :] = jnp.sum(totals[part], axis=0, keepdims=True)


def first_kernel(vis_hbm, sky_hbm, flags_hbm, init_hbm, message, previous, vis, sky, flags, init, sums, small_sems, wide_sems):
    row = lax.axis_index("row")
    col = lax.axis_index("col")
    small = [
        pltpu.make_async_copy(flags_hbm, flags, small_sems.at[0]),
        pltpu.make_async_copy(init_hbm, init, small_sems.at[1]),
    ]
    wide = [
        [
            pltpu.make_async_copy(source.at[:, :, j], target.at[j], wide_sems.at[which, j])
            for which, (source, target) in enumerate(((vis_hbm, vis), (sky_hbm, sky)))
        ]
        for j in range(4)
    ]
    for copy in small + sum(wide, []):
        copy.start()

    long = lax.broadcasted_iota(jnp.int32, (HALF, HALF * TIMES), 1)
    short = lax.broadcasted_iota(jnp.int32, (HALF, HALF * TIMES), 0)
    chosen = jnp.where(lax.shift_right_logical(long, 3) == short, 1.0, 0.0).astype(jnp.bfloat16)
    for copy in small:
        copy.wait()
    low = low_lanes(4)

    def block(ref, index, lead):
        start = pl.multiple_of(lax.shift_right_logical(index, 1) * 128, 128)
        return own_half(ref[lead + (slice(None), pl.ds(start, 128))], lax.rem(index, 2) == 1)

    def wide_gains(index):
        parts = []
        for part in range(2):
            mine = block(init, index, (part,))
            parts.append(jnp.where(low, mine[:4], swap(mine)[4:]))
        return jnp.concatenate(parts, axis=0)

    previous[...] = pack(wide_gains(row), col)
    gain_re, gain_im = spread(wide_gains(col))
    row_flag = block(flags, row, ()).astype(F32)
    row_flag = jnp.where(low_lanes(1), row_flag, swap(row_flag))
    col_flag = jnp.broadcast_to(block(flags, col, ()).astype(F32), (8, 128)).T[:HALF, 0:1]
    col_ids = col * HALF + lax.broadcasted_iota(jnp.int32, (HALF, 128), 0)
    row_ids = row * HALF + (lax.broadcasted_iota(jnp.int32, (HALF, 128), 1) & (HALF - 1))
    scale = jnp.where(col_ids != row_ids, col_flag * row_flag, 0.0)

    def time_total(value):
        high = value.astype(jnp.bfloat16)
        rest = (value - high.astype(F32)).astype(jnp.bfloat16)
        dims = (((1,), (1,)), ((), ()))
        total = lax.dot_general(chosen, high, dims, preferred_element_type=F32)
        return total + lax.dot_general(chosen, rest, dims, preferred_element_type=F32)

    for j in range(4):
        for copy in wide[j]:
            copy.wait()

        def wide_part(ref, part):
            return ref[j, part].reshape(128, HALF * TIMES).astype(F32)

        vis_re, vis_im = wide_part(vis, 0), wide_part(vis, 1)
        mod_re, mod_im = wide_part(sky, 0), wide_part(sky, 1)
        cross_re = time_total(vis_re * mod_re + vis_im * mod_im) * scale
        cross_im = time_total(vis_im * mod_re - vis_re * mod_im) * scale
        power = time_total(mod_re * mod_re + mod_im * mod_im) * scale
        for part, value in enumerate((cross_re, cross_im, power)):
            for peer in range(PEERS):
                at = (part * 4 + j) * 8
                message[peer, at : at + 8] = value[peer * 8 : peer * 8 + 8]
        rows = products(cross_re, cross_im, power, gain_re[j], gain_im[j])
        for part in range(3):
            sums[part * 4 + j : part * 4 + j + 1, :] = rows[part]
    sums[12:16, :] = jnp.zeros((4, 128), F32)
    for peer in range(PEERS):
        message[peer, TILE_ROWS:] = sums[...]


def updated_gains(numerator, denominator, previous):
    return 0.5 * (numerator / (denominator + 1.0) + previous)


def twice(rows):
    return jnp.concatenate([rows, rows], axis=0)


def update_kernel(start, received, previous, message):
    summed = jnp.sum(received[:, start : start + 16], axis=0)
    col = lax.axis_index("col")
    updated = updated_gains(pack(summed[0:8], col), pack(twice(summed[8:12]), col), previous[...])
    message[...] = jnp.broadcast_to(updated, message.shape)


def iterate_kernel(updated, tile, message, previous, gains_of, sums):
    gains = smoothed(updated, lax.axis_index("sub"))
    gains_of[...] = gains
    previous[...] = gains_of[pl.ds(lax.axis_index("row"), 1), :]
    contract(tile, gains, sums)
    sums[12:13, :] = previous[...]
    sums[13:16, :] = jnp.zeros((3, 128), F32)
    for peer in range(PEERS):
        message[peer] = sums[...]


def last_update_kernel(received, message):
    summed = jnp.sum(received[:, 0:12], axis=0)
    previous = jnp.concatenate([received[peer, 12:13] for peer in range(PEERS)], axis=0)
    updated = updated_gains(pack_all(summed[0:8]), pack_all(twice(summed[8:12])), previous)
    for peer in range(PEERS):
        message[peer] = updated


def share_kernel(updated, message):
    gains = unpack(smoothed(updated, lax.axis_index("sub")))
    for peer in range(PEERS):
        message[peer] = gains


def collect_kernel(received, out):
    low = low_lanes(4)
    for part in range(2):
        for pair in range(4):
            even = received[2 * pair, part * 4 : part * 4 + 4]
            odd = received[2 * pair + 1, part * 4 : part * 4 + 4]
            out[part, 0:4, pair * 128 : pair * 128 + 128] = jnp.where(low, even, swap(odd))
            out[part, 4:8, pair * 128 : pair * 128 + 128] = jnp.where(low, swap(even), odd)


def shaped(*shape):
    return jax.ShapeDtypeStruct(shape, F32)


def call(name, kernel, outs, *args, scratch=()):
    return pl.pallas_call(
        kernel,
        out_shape=outs,
        in_specs=[VMEM] * len(args),
        out_specs=jax.tree.map(lambda _: VMEM, outs),
        scratch_shapes=scratch,
        compiler_params=pltpu.CompilerParams(vmem_limit_bytes=4 << 20),
        name=name,
    )(*args)


def exchange(message, axis):
    return lax.all_to_all(message, axis, 0, 0, tiled=True)


def body(visibility, sky_model, antenna_flags, gains_init):
    wide = (2, 2, 4, HALF, HALF * TIMES)
    stay = pl.BlockSpec(memory_space=pl.ANY)
    message, previous = pl.pallas_call(
        first_kernel,
        out_shape=(shaped(PEERS, TILE_ROWS + 16, 128), shaped(1, 128)),
        in_specs=[stay] * 4,
        out_specs=(VMEM, VMEM),
        scratch_shapes=[
            pltpu.VMEM((4, 2, 2, HALF, HALF * TIMES), jnp.bfloat16),
            pltpu.VMEM((4, 2, 2, HALF, HALF * TIMES), jnp.bfloat16),
            pltpu.VMEM((1, 512), jnp.int32),
            pltpu.VMEM((2, 8, 512), F32),
            pltpu.VMEM((16, 128), F32),
            pltpu.SemaphoreType.DMA((2,)),
            pltpu.SemaphoreType.DMA((2, 4)),
        ],
        compiler_params=pltpu.CompilerParams(vmem_limit_bytes=FIRST_LIMIT),
        name="first_kernel",
    )(
        *[
            pltpu.with_memory_space_constraint(value, pltpu.HBM)
            for value in (visibility.reshape(wide), sky_model.reshape(wide), antenna_flags, gains_init)
        ]
    )
    tile = received = exchange(message, "col")
    scratch = [pltpu.VMEM((8, 128), F32), pltpu.VMEM((16, 128), F32)]
    for start in (TILE_ROWS, 0):
        kernel = functools.partial(update_kernel, start)
        message = call("update_kernel", kernel, shaped(PEERS * PEERS, 128), received, previous)
        updated = exchange(message, ("sub", "row")).reshape(PEERS, PEERS, 128)
        outs = (shaped(PEERS, 16, 128), shaped(1, 128))
        message, previous = call("iterate_kernel", iterate_kernel, outs, updated, tile, scratch=scratch)
        received = exchange(message, "col")
    message = call("last_update_kernel", last_update_kernel, shaped(PEERS, 8, 128), received)
    updated = exchange(message, "sub")
    message = call("share_kernel", share_kernel, shaped(PEERS, 8, 128), updated)
    received = exchange(message, "row")
    return call("collect_kernel", collect_kernel, shaped(2, 8, 512), received)


def solution(mesh):
    return jax.shard_map(
        body,
        mesh=mesh,
        in_specs=(
            P(None, "sub", "row", "col"),
            P(None, "sub", "row", "col"),
            P("sub", None),
            P(None, "sub", None),
        ),
        out_specs=P(None, "sub", None),
        check_vma=False,
    )
```

```python
import functools

import jax
import jax.numpy as jnp
from jax import lax
from jax.experimental import pallas as pl
from jax.experimental.pallas import tpu as pltpu
from jax.sharding import PartitionSpec as P


TIMES = 8
PEERS = 8
HALF = 64
F32 = jnp.float32
FIRST_LIMIT = 16 << 20
TILE_ROWS = 96
VMEM = pl.BlockSpec(memory_space=pltpu.VMEM)


def low_lanes(rows):
    return lax.broadcasted_iota(jnp.int32, (rows, 128), 1) < HALF


def swap(value):
    return pltpu.roll(value, HALF, 1)


def own_half(slab, odd):
    return jnp.where(odd, swap(slab), slab)


def spread_row(turned, row):
    first = jnp.broadcast_to(turned[:HALF, row : row + 1], (HALF, 128))
    second = jnp.broadcast_to(turned[HALF:, row : row + 1], (HALF, 128))
    return jnp.where(low_lanes(HALF), first, second)


def products(cross_re, cross_im, power, gain_re, gain_im):
    over = lambda value: jnp.sum(value, axis=0, keepdims=True)
    return (
        over(cross_re * gain_re - cross_im * gain_im),
        over(cross_re * gain_im + cross_im * gain_re),
        over(power * (gain_re * gain_re + gain_im * gain_im)),
    )


def lanes_of(rows):
    return lax.broadcasted_iota(jnp.int32, (rows, 128), 1)


def slide(value, step):
    line = lax.broadcasted_iota(jnp.int32, (8, 128), 0)
    out = value
    for row in range(1, 8):
        out = jnp.where(line == row, pltpu.roll(value, (step * row) % 128, 1), out)
    return out


def pack_all(wide):
    lane = lanes_of(8)
    own = lax.shift_right_logical(lane, 4) == lax.broadcasted_iota(jnp.int32, (8, 128), 0)
    near = own & ((lane & 8) == 0)
    far = own & ((lane & 8) != 0)
    moved = slide(wide, 16)
    rows = []
    for which in range(8):
        first = pltpu.roll(moved, (128 - 8 * which) % 128, 1)
        second = pltpu.roll(moved, (200 - 8 * which) % 128, 1)
        value = jnp.where(near, first, jnp.where(far, second, 0.0))
        rows.append(jnp.sum(value, axis=0, keepdims=True))
    return rows


def unpack(packed, which):
    group = lax.shift_right_logical(lanes_of(8), 3)
    moved = slide(jnp.broadcast_to(packed, (8, 128)), 112)
    first = pltpu.roll(moved, 8 * which, 1)
    second = pltpu.roll(moved, (8 * which + 56) % 128, 1)
    return jnp.where(group == which, first, jnp.where(group == which + 8, second, 0.0))


def channel_mean(packed):
    lane = lanes_of(8) & (HALF - 1)
    total = packed
    for step in range(8, HALF, 8):
        total = total + jnp.where(lane >= step, pltpu.roll(packed, step, 1), pltpu.roll(packed, step + HALF, 1))
    return total / 8.0


def smoothed(updated, sub):
    overall = jnp.sum(updated[...], axis=0) / 8.0
    own = updated[sub]
    return own + 0.5 * channel_mean(overall - own)


def spread_packed(gains):
    turned = gains.T
    low = low_lanes(8)
    columns = []
    for row in range(8):
        pieces = []
        for which in range(8):
            first = jnp.broadcast_to(turned[row * 16 : row * 16 + 8, which : which + 1], (8, 128))
            second = jnp.broadcast_to(turned[row * 16 + 8 : row * 16 + 16, which : which + 1], (8, 128))
            pieces.append(jnp.where(low, first, second))
        columns.append(pieces)
    return columns[:4], columns[4:]


def contract(tile, gains, sums):
    gain_re, gain_im = spread_packed(gains)
    for j in range(4):
        totals = [jnp.zeros((8, 128), F32)] * 3
        for which in range(8):
            cross_re, cross_im, power = [
                tile[which, (part * 4 + j) * 8 : (part * 4 + j) * 8 + 8] for part in range(3)
            ]
            re, im = gain_re[j][which], gain_im[j][which]
            totals[0] += cross_re * re - cross_im * im
            totals[1] += cross_re * im + cross_im * re
            totals[2] += power * (re * re + im * im)
        for part in range(3):
            sums[part * 4 + j : part * 4 + j + 1, :] = jnp.sum(totals[part], axis=0, keepdims=True)


def twice(rows):
    return jnp.concatenate([rows, rows], axis=0)


def share_sums(summed, message, start):
    numerators = pack_all(summed[0:8])
    denominators = pack_all(twice(summed[8:12]))
    for peer in range(PEERS):
        rows = [numerators[peer], denominators[peer], jnp.zeros((6, 128), F32)]
        message[peer, start : start + 8] = jnp.concatenate(rows, axis=0)


def first_kernel(vis_hbm, sky_hbm, flags_hbm, init_hbm, message, previous, vis, sky, flags, init, parts, gain, sums, small_sems, wide_sems):
    row = lax.axis_index("row")
    col = lax.axis_index("col")
    small = [
        pltpu.make_async_copy(flags_hbm, flags, small_sems.at[0]),
        pltpu.make_async_copy(init_hbm, init, small_sems.at[1]),
    ]
    wide = [
        [
            pltpu.make_async_copy(source.at[:, :, j], target.at[j], wide_sems.at[which, j])
            for which, (source, target) in enumerate(((vis_hbm, vis), (sky_hbm, sky)))
        ]
        for j in range(4)
    ]
    for copy in small + sum(wide, []):
        copy.start()

    long = lax.broadcasted_iota(jnp.int32, (HALF, HALF * TIMES), 1)
    short = lax.broadcasted_iota(jnp.int32, (HALF, HALF * TIMES), 0)
    chosen = jnp.where(lax.shift_right_logical(long, 3) == short, 1.0, 0.0).astype(jnp.bfloat16)
    for copy in small + wide[0]:
        copy.wait()
    low = low_lanes(4)

    def block(ref, index, lead):
        start = pl.multiple_of(lax.shift_right_logical(index, 1) * 128, 128)
        return own_half(ref[lead + (slice(None), pl.ds(start, 128))], lax.rem(index, 2) == 1)

    def wide_gains(index):
        parts = []
        for part in range(2):
            mine = block(init, index, (part,))
            parts.append(jnp.where(low, mine[:4], swap(mine)[4:]))
        return jnp.concatenate(parts, axis=0)

    mine = pack_all(wide_gains(row))
    chosen_row = mine[0]
    for which in range(1, 8):
        chosen_row = jnp.where(col == which, mine[which], chosen_row)
    previous[...] = chosen_row
    row_flag = block(flags, row, ()).astype(F32)
    row_flag = jnp.where(low_lanes(1), row_flag, swap(row_flag))
    col_flag = jnp.broadcast_to(block(flags, col, ()).astype(F32), (8, 128)).T[:HALF, 0:1]
    col_ids = col * HALF + lax.broadcasted_iota(jnp.int32, (HALF, 128), 0)
    row_ids = row * HALF + (lax.broadcasted_iota(jnp.int32, (HALF, 128), 1) & (HALF - 1))
    scale = jnp.where(col_ids != row_ids, col_flag * row_flag, 0.0)

    dims = (((1,), (1,)), ((), ()))

    def split(j, piece):
        half, at, lanes = piece // 8, piece // 2 % 4 * 16, pl.ds(piece % 2 * 256, 256)
        rows = pl.ds(half * HALF + at, 16)
        vis_re, vis_im = [vis[j, part, half, pl.ds(at, 16), lanes].astype(F32) for part in range(2)]
        mod_re, mod_im = [sky[j, part, half, pl.ds(at, 16), lanes].astype(F32) for part in range(2)]
        values = (
            vis_re * mod_re + vis_im * mod_im,
            vis_im * mod_re - vis_re * mod_im,
            mod_re * mod_re + mod_im * mod_im,
        )
        for which, value in enumerate(values):
            high = value.astype(jnp.bfloat16)
            parts[j % 2, 2 * which, rows, lanes] = high
            parts[j % 2, 2 * which + 1, rows, lanes] = (value - high.astype(F32)).astype(jnp.bfloat16)

    def time_total(j, which):
        high = lax.dot_general(chosen, parts[j % 2, 2 * which], dims, preferred_element_type=F32)
        rest = lax.dot_general(chosen, parts[j % 2, 2 * which + 1], dims, preferred_element_type=F32)
        value = (high + rest) * scale
        for peer in range(PEERS):
            at = (which * 4 + j) * 8
            message[peer, at : at + 8] = value[peer * 8 : peer * 8 + 8]
        return value

    turned = wide_gains(col).T
    for step in range(5):
        totals = []
        if 0 < step < 4:
            for copy in wide[step]:
                copy.wait()
        for piece in range(16):
            if step < 4:
                split(step, piece)
            if step == 0 and piece % 2 == 1:
                gain[piece // 2] = spread_row(turned, piece // 2)
            if step > 0 and piece in (3, 8, 13):
                totals.append(time_total(step - 1, len(totals)))
        if step > 0:
            j = step - 1
            rows = products(*totals, gain[j], gain[4 + j])
            for part in range(3):
                sums[part * 4 + j : part * 4 + j + 1, :] = rows[part]
    share_sums(sums[...], message, TILE_ROWS)


def update_kernel(start, received, previous, message):
    summed = jnp.sum(received[:, start : start + 8], axis=0)
    updated = 0.5 * (summed[0:1] / (summed[1:2] + 1.0) + previous[...])
    message[...] = jnp.broadcast_to(updated, message.shape)


def iterate_kernel(updated, tile, message, previous, gains_of, sums):
    gains = smoothed(updated, lax.axis_index("sub"))
    gains_of[...] = gains
    previous[...] = gains_of[pl.ds(lax.axis_index("row"), 1), :]
    contract(tile, gains, sums)
    share_sums(sums[...], message, 0)


def last_iterate_kernel(updated, tile, message, gains_of, sums):
    gains = smoothed(updated, lax.axis_index("sub"))
    gains_of[...] = gains
    own = unpack(gains_of[pl.ds(lax.axis_index("row"), 1), :], lax.axis_index("col"))
    contract(tile, gains, sums)
    for peer in range(PEERS):
        message[peer, 0:12] = sums[0:12, :]
        message[peer, 12:20] = own
        message[peer, 20:24] = jnp.zeros((4, 128), F32)


def last_update_kernel(received, mean, rest):
    summed = jnp.sum(received[...], axis=0)
    quotient = summed[0:8] / (twice(summed[8:12]) + 1.0)
    updated = 0.5 * (quotient + summed[12:20])
    means = []
    kept = []
    for part in range(2):
        values = updated[part * 4 : part * 4 + 4]
        total = jnp.sum(values, axis=0, keepdims=True)
        total = (total + swap(total)) / 8.0
        means.append(total)
        kept.append(values - 0.5 * total)
    mean[...] = jnp.broadcast_to(jnp.where(low_lanes(1), means[0], means[1]), (PEERS, 128))
    rest[...] = jnp.concatenate(kept, axis=0)


def share_kernel(means, rest, message):
    overall = jnp.sum(means[...], axis=0, keepdims=True) / 16.0
    other = swap(overall)
    low = low_lanes(1)
    gains = jnp.concatenate(
        [rest[0:4] + jnp.where(low, overall, other), rest[4:8] + jnp.where(low, other, overall)], axis=0
    )
    for peer in range(PEERS):
        message[peer] = gains


def collect_kernel(received, out):
    low = low_lanes(4)
    for part in range(2):
        for pair in range(4):
            even = received[2 * pair, part * 4 : part * 4 + 4]
            odd = received[2 * pair + 1, part * 4 : part * 4 + 4]
            out[part, 0:4, pair * 128 : pair * 128 + 128] = jnp.where(low, even, swap(odd))
            out[part, 4:8, pair * 128 : pair * 128 + 128] = jnp.where(low, swap(even), odd)


def shaped(*shape):
    return jax.ShapeDtypeStruct(shape, F32)


def call(name, kernel, outs, *args, scratch=()):
    return pl.pallas_call(
        kernel,
        out_shape=outs,
        in_specs=[VMEM] * len(args),
        out_specs=jax.tree.map(lambda _: VMEM, outs),
        scratch_shapes=scratch,
        compiler_params=pltpu.CompilerParams(vmem_limit_bytes=4 << 20),
        name=name,
    )(*args)


def exchange(message, axis):
    return lax.all_to_all(message, axis, 0, 0, tiled=True)


def body(visibility, sky_model, antenna_flags, gains_init):
    wide = (2, 2, 4, HALF, HALF * TIMES)
    stay = pl.BlockSpec(memory_space=pl.ANY)
    message, previous = pl.pallas_call(
        first_kernel,
        out_shape=(shaped(PEERS, TILE_ROWS + 8, 128), shaped(1, 128)),
        in_specs=[stay] * 4,
        out_specs=(VMEM, VMEM),
        scratch_shapes=[
            pltpu.VMEM((4, 2, 2, HALF, HALF * TIMES), jnp.bfloat16),
            pltpu.VMEM((4, 2, 2, HALF, HALF * TIMES), jnp.bfloat16),
            pltpu.VMEM((1, 512), jnp.int32),
            pltpu.VMEM((2, 8, 512), F32),
            pltpu.VMEM((2, 6, 128, HALF * TIMES), jnp.bfloat16),
            pltpu.VMEM((8, HALF, 128), F32),
            pltpu.VMEM((16, 128), F32),
            pltpu.SemaphoreType.DMA((2,)),
            pltpu.SemaphoreType.DMA((2, 4)),
        ],
        compiler_params=pltpu.CompilerParams(vmem_limit_bytes=FIRST_LIMIT),
        name="first_kernel",
    )(
        *[
            pltpu.with_memory_space_constraint(value, pltpu.HBM)
            for value in (visibility.reshape(wide), sky_model.reshape(wide), antenna_flags, gains_init)
        ]
    )
    tile = received = exchange(message, "col")
    scratch = [pltpu.VMEM((8, 128), F32), pltpu.VMEM((16, 128), F32)]
    for step in range(2):
        kernel = functools.partial(update_kernel, 0 if step else TILE_ROWS)
        message = call("update_kernel", kernel, shaped(PEERS * PEERS, 128), received, previous)
        updated = exchange(message, ("sub", "row")).reshape(PEERS, PEERS, 128)
        if step == 0:
            outs = (shaped(PEERS, 8, 128), shaped(1, 128))
            message, previous = call("iterate_kernel", iterate_kernel, outs, updated, tile, scratch=scratch)
        else:
            outs = shaped(PEERS, 24, 128)
            message = call("last_iterate_kernel", last_iterate_kernel, outs, updated, tile, scratch=scratch)
        received = exchange(message, "col")
    outs = (shaped(PEERS, 128), shaped(8, 128))
    mean, rest = call("last_update_kernel", last_update_kernel, outs, received)
    means = exchange(mean, "sub")
    message = call("share_kernel", share_kernel, shaped(PEERS, 8, 128), means, rest)
    received = exchange(message, "row")
    return call("collect_kernel", collect_kernel, shaped(2, 8, 512), received)


def solution(mesh):
    return jax.shard_map(
        body,
        mesh=mesh,
        in_specs=(
            P(None, "sub", "row", "col"),
            P(None, "sub", "row", "col"),
            P("sub", None),
            P(None, "sub", None),
        ),
        out_specs=P(None, "sub", None),
        check_vma=False,
    )
```

```python
import functools

import jax
import jax.numpy as jnp
from jax import lax
from jax.experimental import pallas as pl
from jax.experimental.pallas import tpu as pltpu
from jax.sharding import PartitionSpec as P


TIMES = 8
PEERS = 8
HALF = 64
F32 = jnp.float32
FIRST_LIMIT = 16 << 20
TILE_ROWS = 96
VMEM = pl.BlockSpec(memory_space=pltpu.VMEM)


def low_lanes(rows):
    return lax.broadcasted_iota(jnp.int32, (rows, 128), 1) < HALF


def swap(value):
    return pltpu.roll(value, HALF, 1)


def own_half(slab, odd):
    return jnp.where(odd, swap(slab), slab)


def spread_row(turned, row):
    first = jnp.broadcast_to(turned[:HALF, row : row + 1], (HALF, 128))
    second = jnp.broadcast_to(turned[HALF:, row : row + 1], (HALF, 128))
    return jnp.where(low_lanes(HALF), first, second)


def products(cross_re, cross_im, power, gain_re, gain_im):
    over = lambda value: jnp.sum(value, axis=0, keepdims=True)
    return (
        over(cross_re * gain_re - cross_im * gain_im),
        over(cross_re * gain_im + cross_im * gain_re),
        over(power * (gain_re * gain_re + gain_im * gain_im)),
    )


def lanes_of(rows):
    return lax.broadcasted_iota(jnp.int32, (rows, 128), 1)


def slide(value, step):
    line = lax.broadcasted_iota(jnp.int32, (8, 128), 0)
    out = value
    for row in range(1, 8):
        out = jnp.where(line == row, pltpu.roll(value, (step * row) % 128, 1), out)
    return out


def pack_all(wide):
    lane = lanes_of(8)
    own = lax.shift_right_logical(lane, 4) == lax.broadcasted_iota(jnp.int32, (8, 128), 0)
    near = own & ((lane & 8) == 0)
    far = own & ((lane & 8) != 0)
    moved = slide(wide, 16)
    rows = []
    for which in range(8):
        first = pltpu.roll(moved, (128 - 8 * which) % 128, 1)
        second = pltpu.roll(moved, (200 - 8 * which) % 128, 1)
        value = jnp.where(near, first, jnp.where(far, second, 0.0))
        rows.append(jnp.sum(value, axis=0, keepdims=True))
    return rows


def unpack(packed, which):
    group = lax.shift_right_logical(lanes_of(8), 3)
    moved = slide(jnp.broadcast_to(packed, (8, 128)), 112)
    first = pltpu.roll(moved, 8 * which, 1)
    second = pltpu.roll(moved, (8 * which + 56) % 128, 1)
    return jnp.where(group == which, first, jnp.where(group == which + 8, second, 0.0))


def channel_mean(packed):
    lane = lanes_of(8) & (HALF - 1)
    total = packed
    for step in range(8, HALF, 8):
        total = total + jnp.where(lane >= step, pltpu.roll(packed, step, 1), pltpu.roll(packed, step + HALF, 1))
    return total / 8.0


def smoothed(updated, sub):
    overall = jnp.sum(updated[...], axis=0) / 8.0
    own = updated[sub]
    return own + 0.5 * channel_mean(overall - own)


def spread_packed(gains):
    turned = gains.T
    low = low_lanes(8)
    columns = []
    for row in range(8):
        pieces = []
        for which in range(8):
            first = jnp.broadcast_to(turned[row * 16 : row * 16 + 8, which : which + 1], (8, 128))
            second = jnp.broadcast_to(turned[row * 16 + 8 : row * 16 + 16, which : which + 1], (8, 128))
            pieces.append(jnp.where(low, first, second))
        columns.append(pieces)
    return columns[:4], columns[4:]


def contract(tile, gains, sums):
    gain_re, gain_im = spread_packed(gains)
    for j in range(4):
        totals = [jnp.zeros((8, 128), F32)] * 3
        for which in range(8):
            cross_re, cross_im, power = [
                tile[which, (part * 4 + j) * 8 : (part * 4 + j) * 8 + 8] for part in range(3)
            ]
            re, im = gain_re[j][which], gain_im[j][which]
            totals[0] += cross_re * re - cross_im * im
            totals[1] += cross_re * im + cross_im * re
            totals[2] += power * (re * re + im * im)
        for part in range(3):
            sums[part * 4 + j : part * 4 + j + 1, :] = jnp.sum(totals[part], axis=0, keepdims=True)


def twice(rows):
    return jnp.concatenate([rows, rows], axis=0)


def share_sums(summed, message, start):
    numerators = pack_all(summed[0:8])
    denominators = pack_all(twice(summed[8:12]))
    for peer in range(PEERS):
        message[peer, start : start + 1] = numerators[peer]
        message[peer, start + 1 : start + 2] = denominators[peer]


def first_kernel(vis_hbm, sky_hbm, flags_hbm, init_hbm, message, previous, vis, sky, flags, init, parts, gain, sums, small_sems, wide_sems):
    row = lax.axis_index("row")
    col = lax.axis_index("col")
    small = [
        pltpu.make_async_copy(flags_hbm, flags, small_sems.at[0]),
        pltpu.make_async_copy(init_hbm, init, small_sems.at[1]),
    ]
    wide = [
        [
            pltpu.make_async_copy(source.at[:, :, j], target.at[j], wide_sems.at[which, j])
            for which, (source, target) in enumerate(((vis_hbm, vis), (sky_hbm, sky)))
        ]
        for j in range(4)
    ]
    for copy in small + sum(wide, []):
        copy.start()

    long = lax.broadcasted_iota(jnp.int32, (HALF, HALF * TIMES), 1)
    short = lax.broadcasted_iota(jnp.int32, (HALF, HALF * TIMES), 0)
    chosen = jnp.where(lax.shift_right_logical(long, 3) == short, 1.0, 0.0).astype(jnp.bfloat16)
    for copy in small:
        copy.wait()
    low = low_lanes(4)

    def block(ref, index, lead):
        start = pl.multiple_of(lax.shift_right_logical(index, 1) * 128, 128)
        return own_half(ref[lead + (slice(None), pl.ds(start, 128))], lax.rem(index, 2) == 1)

    def wide_gains(index):
        parts = []
        for part in range(2):
            mine = block(init, index, (part,))
            parts.append(jnp.where(low, mine[:4], swap(mine)[4:]))
        return jnp.concatenate(parts, axis=0)

    mine = pack_all(wide_gains(row))
    chosen_row = mine[0]
    for which in range(1, 8):
        chosen_row = jnp.where(col == which, mine[which], chosen_row)
    previous[...] = chosen_row
    row_flag = block(flags, row, ()).astype(F32)
    row_flag = jnp.where(low_lanes(1), row_flag, swap(row_flag))
    col_flag = jnp.broadcast_to(block(flags, col, ()).astype(F32), (8, 128)).T[:HALF, 0:1]
    col_ids = col * HALF + lax.broadcasted_iota(jnp.int32, (HALF, 128), 0)
    row_ids = row * HALF + (lax.broadcasted_iota(jnp.int32, (HALF, 128), 1) & (HALF - 1))
    scale = jnp.where(col_ids != row_ids, col_flag * row_flag, 0.0)

    dims = (((1,), (1,)), ((), ()))

    def split(j, piece):
        half, at, lanes = piece // 8, piece // 2 % 4 * 16, pl.ds(piece % 2 * 256, 256)
        rows = pl.ds(half * HALF + at, 16)
        vis_re, vis_im = [vis[j, part, half, pl.ds(at, 16), lanes].astype(F32) for part in range(2)]
        mod_re, mod_im = [sky[j, part, half, pl.ds(at, 16), lanes].astype(F32) for part in range(2)]
        values = (
            vis_re * mod_re + vis_im * mod_im,
            vis_im * mod_re - vis_re * mod_im,
            mod_re * mod_re + mod_im * mod_im,
        )
        for which, value in enumerate(values):
            high = value.astype(jnp.bfloat16)
            parts[j % 2, 2 * which, rows, lanes] = high
            parts[j % 2, 2 * which + 1, rows, lanes] = (value - high.astype(F32)).astype(jnp.bfloat16)

    def time_total(j, which):
        high = lax.dot_general(chosen, parts[j % 2, 2 * which], dims, preferred_element_type=F32)
        rest = lax.dot_general(chosen, parts[j % 2, 2 * which + 1], dims, preferred_element_type=F32)
        value = (high + rest) * scale
        for peer in range(PEERS):
            at = (which * 4 + j) * 8
            message[peer, at : at + 8] = value[peer * 8 : peer * 8 + 8]
        return value

    turned = wide_gains(col).T
    for line in range(8):
        gain[line] = spread_row(turned, line)
    for step in range(5):
        totals = []
        if step < 2:
            for copy in (wide[0] if step == 0 else sum(wide[1:], [])):
                copy.wait()
        for piece in range(16):
            if step < 4:
                split(step, piece)
            if step > 0 and piece in (3, 8, 13):
                totals.append(time_total(step - 1, len(totals)))
        if step > 0:
            j = step - 1
            rows = products(*totals, gain[j], gain[4 + j])
            for part in range(3):
                sums[part * 4 + j : part * 4 + j + 1, :] = rows[part]
    share_sums(sums[...], message, TILE_ROWS)


def update_kernel(start, received, previous, message):
    summed = jnp.sum(received[:, start : start + 2], axis=0)
    updated = 0.5 * (summed[0:1] / (summed[1:2] + 1.0) + previous[...])
    message[...] = jnp.broadcast_to(updated, message.shape)


def iterate_kernel(updated, tile, message, previous, gains_of, sums):
    gains = smoothed(updated, lax.axis_index("sub"))
    gains_of[...] = gains
    previous[...] = gains_of[pl.ds(lax.axis_index("row"), 1), :]
    contract(tile, gains, sums)
    share_sums(sums[...], message, 0)


def last_iterate_kernel(updated, tile, message, gains_of, sums):
    gains = smoothed(updated, lax.axis_index("sub"))
    gains_of[...] = gains
    own = unpack(gains_of[pl.ds(lax.axis_index("row"), 1), :], lax.axis_index("col"))
    contract(tile, gains, sums)
    for peer in range(PEERS):
        message[peer, 0:12] = sums[0:12, :]
        message[peer, 12:20] = own


def last_update_kernel(received, mean, rest):
    summed = jnp.sum(received[...], axis=0)
    quotient = summed[0:8] / (twice(summed[8:12]) + 1.0)
    updated = 0.5 * (quotient + summed[12:20])
    means = []
    kept = []
    for part in range(2):
        values = updated[part * 4 : part * 4 + 4]
        total = jnp.sum(values, axis=0, keepdims=True)
        total = (total + swap(total)) / 8.0
        means.append(total)
        kept.append(values - 0.5 * total)
    mean[...] = jnp.broadcast_to(jnp.where(low_lanes(1), means[0], means[1]), (PEERS, 128))
    rest[...] = jnp.concatenate(kept, axis=0)


def share_kernel(means, rest, message):
    overall = jnp.sum(means[...], axis=0, keepdims=True) / 16.0
    other = swap(overall)
    low = low_lanes(1)
    gains = jnp.concatenate(
        [rest[0:4] + jnp.where(low, overall, other), rest[4:8] + jnp.where(low, other, overall)], axis=0
    )
    for peer in range(PEERS):
        message[peer] = gains


def collect_kernel(received, out):
    low = low_lanes(4)
    for part in range(2):
        for pair in range(4):
            even = received[2 * pair, part * 4 : part * 4 + 4]
            odd = received[2 * pair + 1, part * 4 : part * 4 + 4]
            out[part, 0:4, pair * 128 : pair * 128 + 128] = jnp.where(low, even, swap(odd))
            out[part, 4:8, pair * 128 : pair * 128 + 128] = jnp.where(low, swap(even), odd)


def shaped(*shape):
    return jax.ShapeDtypeStruct(shape, F32)


def call(name, kernel, outs, *args, scratch=()):
    return pl.pallas_call(
        kernel,
        out_shape=outs,
        in_specs=[VMEM] * len(args),
        out_specs=jax.tree.map(lambda _: VMEM, outs),
        scratch_shapes=scratch,
        compiler_params=pltpu.CompilerParams(vmem_limit_bytes=4 << 20),
        name=name,
    )(*args)


def exchange(message, axis):
    return lax.all_to_all(message, axis, 0, 0, tiled=True)


def body(visibility, sky_model, antenna_flags, gains_init):
    wide = (2, 2, 4, HALF, HALF * TIMES)
    stay = pl.BlockSpec(memory_space=pl.ANY)
    message, previous = pl.pallas_call(
        first_kernel,
        out_shape=(shaped(PEERS, TILE_ROWS + 2, 128), shaped(1, 128)),
        in_specs=[stay] * 4,
        out_specs=(VMEM, VMEM),
        scratch_shapes=[
            pltpu.VMEM((4, 2, 2, HALF, HALF * TIMES), jnp.bfloat16),
            pltpu.VMEM((4, 2, 2, HALF, HALF * TIMES), jnp.bfloat16),
            pltpu.VMEM((1, 512), jnp.int32),
            pltpu.VMEM((2, 8, 512), F32),
            pltpu.VMEM((2, 6, 128, HALF * TIMES), jnp.bfloat16),
            pltpu.VMEM((8, HALF, 128), F32),
            pltpu.VMEM((16, 128), F32),
            pltpu.SemaphoreType.DMA((2,)),
            pltpu.SemaphoreType.DMA((2, 4)),
        ],
        compiler_params=pltpu.CompilerParams(vmem_limit_bytes=FIRST_LIMIT),
        name="first_kernel",
    )(
        *[
            pltpu.with_memory_space_constraint(value, pltpu.HBM)
            for value in (visibility.reshape(wide), sky_model.reshape(wide), antenna_flags, gains_init)
        ]
    )
    tile = received = exchange(message, "col")
    scratch = [pltpu.VMEM((8, 128), F32), pltpu.VMEM((16, 128), F32)]
    for step in range(2):
        kernel = functools.partial(update_kernel, 0 if step else TILE_ROWS)
        message = call("update_kernel", kernel, shaped(PEERS * PEERS, 128), received, previous)
        updated = exchange(message, ("sub", "row")).reshape(PEERS, PEERS, 128)
        if step == 0:
            outs = (shaped(PEERS, 2, 128), shaped(1, 128))
            message, previous = call("iterate_kernel", iterate_kernel, outs, updated, tile, scratch=scratch)
        else:
            outs = shaped(PEERS, 20, 128)
            message = call("last_iterate_kernel", last_iterate_kernel, outs, updated, tile, scratch=scratch)
        received = exchange(message, "col")
    outs = (shaped(PEERS, 128), shaped(8, 128))
    mean, rest = call("last_update_kernel", last_update_kernel, outs, received)
    means = exchange(mean, "sub")
    message = call("share_kernel", share_kernel, shaped(PEERS, 8, 128), means, rest)
    received = exchange(message, "row")
    return call("collect_kernel", collect_kernel, shaped(2, 8, 512), received)


def solution(mesh):
    return jax.shard_map(
        body,
        mesh=mesh,
        in_specs=(
            P(None, "sub", "row", "col"),
            P(None, "sub", "row", "col"),
            P("sub", None),
            P(None, "sub", None),
        ),
        out_specs=P(None, "sub", None),
        check_vma=False,
    )
```

```python
import functools

import jax
import jax.numpy as jnp
from jax import lax
from jax.experimental import pallas as pl
from jax.experimental.pallas import tpu as pltpu
from jax.sharding import PartitionSpec as P


TIMES = 8
PEERS = 8
HALF = 64
F32 = jnp.float32
FIRST_LIMIT = 16 << 20
TILE_ROWS = 96
VMEM = pl.BlockSpec(memory_space=pltpu.VMEM)


def low_lanes(rows):
    return lax.broadcasted_iota(jnp.int32, (rows, 128), 1) < HALF


def swap(value):
    return pltpu.roll(value, HALF, 1)


def own_half(slab, odd):
    return jnp.where(odd, swap(slab), slab)


def spread_row(turned, row):
    first = jnp.broadcast_to(turned[:HALF, row : row + 1], (HALF, 128))
    second = jnp.broadcast_to(turned[HALF:, row : row + 1], (HALF, 128))
    return jnp.where(low_lanes(HALF), first, second)


def products(cross_re, cross_im, power, gain_re, gain_im):
    over = lambda value: jnp.sum(value, axis=0, keepdims=True)
    return (
        over(cross_re * gain_re - cross_im * gain_im),
        over(cross_re * gain_im + cross_im * gain_re),
        over(power * (gain_re * gain_re + gain_im * gain_im)),
    )


def lanes_of(rows):
    return lax.broadcasted_iota(jnp.int32, (rows, 128), 1)


def slide(value, step):
    line = lax.broadcasted_iota(jnp.int32, (8, 128), 0)
    out = value
    for row in range(1, 8):
        out = jnp.where(line == row, pltpu.roll(value, (step * row) % 128, 1), out)
    return out


def pack_all(wide):
    lane = lanes_of(8)
    own = lax.shift_right_logical(lane, 4) == lax.broadcasted_iota(jnp.int32, (8, 128), 0)
    near = own & ((lane & 8) == 0)
    far = own & ((lane & 8) != 0)
    moved = slide(wide, 16)
    rows = []
    for which in range(8):
        first = pltpu.roll(moved, (128 - 8 * which) % 128, 1)
        second = pltpu.roll(moved, (200 - 8 * which) % 128, 1)
        value = jnp.where(near, first, jnp.where(far, second, 0.0))
        rows.append(jnp.sum(value, axis=0, keepdims=True))
    return rows


def unpack(packed, which):
    group = lax.shift_right_logical(lanes_of(8), 3)
    moved = slide(jnp.broadcast_to(packed, (8, 128)), 112)
    first = pltpu.roll(moved, 8 * which, 1)
    second = pltpu.roll(moved, (8 * which + 56) % 128, 1)
    return jnp.where(group == which, first, jnp.where(group == which + 8, second, 0.0))


def channel_mean(packed):
    lane = lanes_of(8) & (HALF - 1)
    total = packed
    for step in range(8, HALF, 8):
        total = total + jnp.where(lane >= step, pltpu.roll(packed, step, 1), pltpu.roll(packed, step + HALF, 1))
    return total / 8.0


def smoothed(updated, sub):
    overall = jnp.sum(updated[...], axis=0) / 8.0
    own = updated[sub]
    return own + 0.5 * channel_mean(overall - own)


def spread_packed(gains):
    turned = gains.T
    low = low_lanes(8)
    columns = []
    for row in range(8):
        pieces = []
        for which in range(8):
            first = jnp.broadcast_to(turned[row * 16 : row * 16 + 8, which : which + 1], (8, 128))
            second = jnp.broadcast_to(turned[row * 16 + 8 : row * 16 + 16, which : which + 1], (8, 128))
            pieces.append(jnp.where(low, first, second))
        columns.append(pieces)
    return columns[:4], columns[4:]


def contract(tile, gains, sums):
    gain_re, gain_im = spread_packed(gains)
    for j in range(4):
        totals = [jnp.zeros((8, 128), F32)] * 3
        for which in range(8):
            cross_re, cross_im, power = [
                tile[which, (part * 4 + j) * 8 : (part * 4 + j) * 8 + 8] for part in range(3)
            ]
            re, im = gain_re[j][which], gain_im[j][which]
            totals[0] += cross_re * re - cross_im * im
            totals[1] += cross_re * im + cross_im * re
            totals[2] += power * (re * re + im * im)
        for part in range(3):
            sums[part * 4 + j : part * 4 + j + 1, :] = jnp.sum(totals[part], axis=0, keepdims=True)


def twice(rows):
    return jnp.concatenate([rows, rows], axis=0)


def share_sums(summed, message, start):
    numerators = pack_all(summed[0:8])
    denominators = pack_all(twice(summed[8:12]))
    for peer in range(PEERS):
        message[peer, start : start + 1] = numerators[peer]
        message[peer, start + 1 : start + 2] = denominators[peer]


def first_kernel(vis_hbm, sky_hbm, flags_hbm, init_hbm, message, previous, vis, sky, flags, init, parts, gain, sums, small_sems, wide_sems):
    row = lax.axis_index("row")
    col = lax.axis_index("col")
    small = [
        pltpu.make_async_copy(flags_hbm, flags, small_sems.at[0]),
        pltpu.make_async_copy(init_hbm, init, small_sems.at[1]),
    ]
    wide = [
        [
            pltpu.make_async_copy(source.at[:, :, j], target.at[j], wide_sems.at[which, j])
            for which, (source, target) in enumerate(((vis_hbm, vis), (sky_hbm, sky)))
        ]
        for j in range(4)
    ]
    for copy in small + sum(wide, []):
        copy.start()

    long = lax.broadcasted_iota(jnp.int32, (HALF, HALF * TIMES), 1)
    short = lax.broadcasted_iota(jnp.int32, (HALF, HALF * TIMES), 0)
    chosen = jnp.where(lax.shift_right_logical(long, 3) == short, 1.0, 0.0).astype(jnp.bfloat16)
    for copy in small:
        copy.wait()
    low = low_lanes(4)

    def block(ref, index, lead):
        start = pl.multiple_of(lax.shift_right_logical(index, 1) * 128, 128)
        return own_half(ref[lead + (slice(None), pl.ds(start, 128))], lax.rem(index, 2) == 1)

    def wide_gains(index):
        parts = []
        for part in range(2):
            mine = block(init, index, (part,))
            parts.append(jnp.where(low, mine[:4], swap(mine)[4:]))
        return jnp.concatenate(parts, axis=0)

    mine = pack_all(wide_gains(row))
    chosen_row = mine[0]
    for which in range(1, 8):
        chosen_row = jnp.where(col == which, mine[which], chosen_row)
    previous[...] = chosen_row
    row_flag = block(flags, row, ()).astype(F32)
    row_flag = jnp.where(low_lanes(1), row_flag, swap(row_flag))
    col_flag = jnp.broadcast_to(block(flags, col, ()).astype(F32), (8, 128)).T[:HALF, 0:1]
    col_ids = col * HALF + lax.broadcasted_iota(jnp.int32, (HALF, 128), 0)
    row_ids = row * HALF + (lax.broadcasted_iota(jnp.int32, (HALF, 128), 1) & (HALF - 1))
    scale = jnp.where(col_ids != row_ids, col_flag * row_flag, 0.0)

    dims = (((1,), (1,)), ((), ()))

    def split(j, piece):
        half, at, lanes = piece // 8, piece // 2 % 4 * 16, pl.ds(piece % 2 * 256, 256)
        rows = pl.ds(half * HALF + at, 16)
        vis_re, vis_im = [vis[j, part, half, pl.ds(at, 16), lanes].astype(F32) for part in range(2)]
        mod_re, mod_im = [sky[j, part, half, pl.ds(at, 16), lanes].astype(F32) for part in range(2)]
        values = (
            vis_re * mod_re + vis_im * mod_im,
            vis_im * mod_re - vis_re * mod_im,
            mod_re * mod_re + mod_im * mod_im,
        )
        for which, value in enumerate(values):
            high = value.astype(jnp.bfloat16)
            parts[j % 2, 2 * which, rows, lanes] = high
            parts[j % 2, 2 * which + 1, rows, lanes] = (value - high.astype(F32)).astype(jnp.bfloat16)

    def time_total(j, which):
        high = lax.dot_general(chosen, parts[j % 2, 2 * which], dims, preferred_element_type=F32)
        rest = lax.dot_general(chosen, parts[j % 2, 2 * which + 1], dims, preferred_element_type=F32)
        value = (high + rest) * scale
        for peer in range(PEERS):
            at = (which * 4 + j) * 8
            message[peer, at : at + 8] = value[peer * 8 : peer * 8 + 8]
        return value

    turned = wide_gains(col).T
    for line in range(8):
        gain[line] = spread_row(turned, line)
    for step in range(5):
        totals = []
        if step < 2:
            for copy in (wide[0] if step == 0 else sum(wide[1:], [])):
                copy.wait()
        for piece in range(16):
            if step < 4:
                split(step, piece)
            if step > 0 and piece in (3, 8, 13):
                totals.append(time_total(step - 1, len(totals)))
        if step > 0:
            j = step - 1
            rows = products(*totals, gain[j], gain[4 + j])
            for part in range(3):
                sums[part * 4 + j : part * 4 + j + 1, :] = rows[part]
    share_sums(sums[...], message, TILE_ROWS)


def update_kernel(start, received, previous, message):
    summed = jnp.sum(received[:, start : start + 2], axis=0)
    updated = 0.5 * (summed[0:1] / (summed[1:2] + 1.0) + previous[...])
    message[...] = jnp.broadcast_to(updated, message.shape)


def iterate_kernel(updated, tile, message, previous, gains_of, sums):
    gains = smoothed(updated, lax.axis_index("sub"))
    gains_of[...] = gains
    previous[...] = gains_of[pl.ds(lax.axis_index("row"), 1), :]
    contract(tile, gains, sums)
    share_sums(sums[...], message, 0)


def last_iterate_kernel(updated, tile, message, gains_of, sums):
    gains = smoothed(updated, lax.axis_index("sub"))
    gains_of[...] = gains
    own = unpack(gains_of[pl.ds(lax.axis_index("row"), 1), :], lax.axis_index("col"))
    contract(tile, gains, sums)
    for peer in range(PEERS):
        message[peer, 0:12] = sums[0:12, :]
        message[peer, 12:20] = own


def last_update_kernel(received, message):
    summed = jnp.sum(received[...], axis=0)
    quotient = summed[0:8] / (twice(summed[8:12]) + 1.0)
    updated = 0.5 * (quotient + summed[12:20])
    means = []
    kept = []
    for part in range(2):
        values = updated[part * 4 : part * 4 + 4]
        total = jnp.sum(values, axis=0, keepdims=True)
        total = (total + swap(total)) / 8.0
        means.append(total)
        kept.append(values - 0.5 * total)
    rest = jnp.concatenate(kept, axis=0)
    mean = jnp.where(low_lanes(1), means[0], means[1])
    for peer in range(PEERS):
        message[peer, 0:8] = rest
        message[peer, 8:9] = mean


def share_kernel(received, message):
    means = jnp.concatenate([received[block, 8:9] for block in range(PEERS)], axis=0)
    for peer in range(PEERS):
        message[peer] = means


def collect_kernel(means, received, out):
    low = low_lanes(4)
    overall = jnp.sum(means[...], axis=0) / 16.0
    other = swap(overall)
    wide = low_lanes(8)
    added = (jnp.where(wide, overall, other), jnp.where(wide, other, overall))
    for part in range(2):
        blocks = [
            received[block, part * 4 : part * 4 + 4] + added[part][block : block + 1] for block in range(PEERS)
        ]
        for pair in range(4):
            even, odd = blocks[2 * pair], blocks[2 * pair + 1]
            out[part, 0:4, pair * 128 : pair * 128 + 128] = jnp.where(low, even, swap(odd))
            out[part, 4:8, pair * 128 : pair * 128 + 128] = jnp.where(low, swap(even), odd)


def shaped(*shape):
    return jax.ShapeDtypeStruct(shape, F32)


def call(name, kernel, outs, *args, scratch=()):
    return pl.pallas_call(
        kernel,
        out_shape=outs,
        in_specs=[VMEM] * len(args),
        out_specs=jax.tree.map(lambda _: VMEM, outs),
        scratch_shapes=scratch,
        compiler_params=pltpu.CompilerParams(vmem_limit_bytes=4 << 20),
        name=name,
    )(*args)


def exchange(message, axis):
    return lax.all_to_all(message, axis, 0, 0, tiled=True)


def body(visibility, sky_model, antenna_flags, gains_init):
    wide = (2, 2, 4, HALF, HALF * TIMES)
    stay = pl.BlockSpec(memory_space=pl.ANY)
    message, previous = pl.pallas_call(
        first_kernel,
        out_shape=(shaped(PEERS, TILE_ROWS + 2, 128), shaped(1, 128)),
        in_specs=[stay] * 4,
        out_specs=(VMEM, VMEM),
        scratch_shapes=[
            pltpu.VMEM((4, 2, 2, HALF, HALF * TIMES), jnp.bfloat16),
            pltpu.VMEM((4, 2, 2, HALF, HALF * TIMES), jnp.bfloat16),
            pltpu.VMEM((1, 512), jnp.int32),
            pltpu.VMEM((2, 8, 512), F32),
            pltpu.VMEM((2, 6, 128, HALF * TIMES), jnp.bfloat16),
            pltpu.VMEM((8, HALF, 128), F32),
            pltpu.VMEM((16, 128), F32),
            pltpu.SemaphoreType.DMA((2,)),
            pltpu.SemaphoreType.DMA((2, 4)),
        ],
        compiler_params=pltpu.CompilerParams(vmem_limit_bytes=FIRST_LIMIT),
        name="first_kernel",
    )(
        *[
            pltpu.with_memory_space_constraint(value, pltpu.HBM)
            for value in (visibility.reshape(wide), sky_model.reshape(wide), antenna_flags, gains_init)
        ]
    )
    tile = received = exchange(message, "col")
    scratch = [pltpu.VMEM((8, 128), F32), pltpu.VMEM((16, 128), F32)]
    for step in range(2):
        kernel = functools.partial(update_kernel, 0 if step else TILE_ROWS)
        message = call("update_kernel", kernel, shaped(PEERS * PEERS, 128), received, previous)
        updated = exchange(message, ("sub", "row")).reshape(PEERS, PEERS, 128)
        if step == 0:
            outs = (shaped(PEERS, 2, 128), shaped(1, 128))
            message, previous = call("iterate_kernel", iterate_kernel, outs, updated, tile, scratch=scratch)
        else:
            outs = shaped(PEERS, 20, 128)
            message = call("last_iterate_kernel", last_iterate_kernel, outs, updated, tile, scratch=scratch)
        received = exchange(message, "col")
    message = call("last_update_kernel", last_update_kernel, shaped(PEERS, 9, 128), received)
    received = exchange(message, "row")
    means = exchange(call("share_kernel", share_kernel, shaped(PEERS, 8, 128), received), "sub")
    return call("collect_kernel", collect_kernel, shaped(2, 8, 512), means, received)


def solution(mesh):
    return jax.shard_map(
        body,
        mesh=mesh,
        in_specs=(
            P(None, "sub", "row", "col"),
            P(None, "sub", "row", "col"),
            P("sub", None),
            P(None, "sub", None),
        ),
        out_specs=P(None, "sub", None),
        check_vma=False,
    )
```

```python
import functools

import jax
import jax.numpy as jnp
from jax import lax
from jax.experimental import pallas as pl
from jax.experimental.pallas import tpu as pltpu
from jax.sharding import PartitionSpec as P


TIMES = 8
PEERS = 8
HALF = 64
F32 = jnp.float32
FIRST_LIMIT = 16 << 20
TILE_ROWS = 96
VMEM = pl.BlockSpec(memory_space=pltpu.VMEM)


def low_lanes(rows):
    return lax.broadcasted_iota(jnp.int32, (rows, 128), 1) < HALF


def swap(value):
    return pltpu.roll(value, HALF, 1)


def own_half(slab, odd):
    return jnp.where(odd, swap(slab), slab)


def beside(gains):
    turned = jnp.concatenate([gains, swap(gains)], axis=0).T
    return jnp.concatenate([turned[:HALF], jnp.zeros((HALF, 112), F32)], axis=1)


def pick(columns, which):
    at = jnp.where(low_lanes(columns.shape[0]), which, which + 8)
    return jnp.take_along_axis(columns, at, axis=1)


def products(cross_re, cross_im, power, gain_re, gain_im):
    over = lambda value: jnp.sum(value, axis=0, keepdims=True)
    return (
        over(cross_re * gain_re - cross_im * gain_im),
        over(cross_re * gain_im + cross_im * gain_re),
        over(power * (gain_re * gain_re + gain_im * gain_im)),
    )


def lanes_of(rows):
    return lax.broadcasted_iota(jnp.int32, (rows, 128), 1)


def slide(value, step):
    line = lax.broadcasted_iota(jnp.int32, (8, 128), 0)
    out = value
    for row in range(1, 8):
        out = jnp.where(line == row, pltpu.roll(value, (step * row) % 128, 1), out)
    return out


def group_of(rows):
    return lax.shift_right_logical(lanes_of(rows) & (HALF - 1), 3)


def pack_all(wide):
    own = group_of(8) == lax.broadcasted_iota(jnp.int32, (8, 128), 0)
    moved = slide(wide, 8)
    rows = []
    for which in range(8):
        value = jnp.where(own, pltpu.roll(moved, (128 - 8 * which) % 128, 1), 0.0)
        rows.append(jnp.sum(value, axis=0, keepdims=True))
    return rows


def channel_mean(packed):
    lane = lanes_of(8) & 31
    total = packed
    for step in (8, 16, 24):
        total = total + jnp.where(lane >= step, pltpu.roll(packed, step, 1), pltpu.roll(packed, step + 96, 1))
    return (total + swap(total)) / 8.0


def smoothed(updated, sub):
    overall = jnp.sum(updated[...], axis=0) / 8.0
    own = updated[sub]
    return own + 0.5 * channel_mean(overall - own)


def contract(tile, gains, sums):
    turned = beside(gains)
    columns = [turned[row * 8 : row * 8 + 8] for row in range(8)]
    totals = [[None] * 3 for _ in range(4)]
    for which in range(8):
        gain = [pick(column, which) for column in columns]
        for j in range(4):
            cross_re, cross_im, power = [
                tile[which, (part * 4 + j) * 8 : (part * 4 + j) * 8 + 8] for part in range(3)
            ]
            re, im = gain[j], gain[4 + j]
            terms = (cross_re * re - cross_im * im, cross_re * im + cross_im * re, power * (re * re + im * im))
            totals[j] = [term if which == 0 else total + term for total, term in zip(totals[j], terms)]
    for j in range(4):
        for part in range(3):
            sums[part * 4 + j : part * 4 + j + 1, :] = jnp.sum(totals[j][part], axis=0, keepdims=True)


def twice(rows):
    return jnp.concatenate([rows, rows], axis=0)


def share_sums(summed, message, start):
    numerators = pack_all(summed[0:8])
    denominators = pack_all(twice(summed[8:12]))
    for peer in range(PEERS):
        message[peer, start : start + 1] = numerators[peer]
        message[peer, start + 1 : start + 2] = denominators[peer]


def first_kernel(vis_hbm, sky_hbm, flags_hbm, init_hbm, message, previous, vis, sky, flags, init, parts, gain, sums, small_sems, wide_sems):
    row = lax.axis_index("row")
    col = lax.axis_index("col")
    small = [
        pltpu.make_async_copy(flags_hbm, flags, small_sems.at[0]),
        pltpu.make_async_copy(init_hbm, init, small_sems.at[1]),
    ]
    wide = [
        [
            pltpu.make_async_copy(source.at[:, :, j], target.at[j], wide_sems.at[which, j])
            for which, (source, target) in enumerate(((vis_hbm, vis), (sky_hbm, sky)))
        ]
        for j in range(4)
    ]
    for copy in small + sum(wide, []):
        copy.start()

    long = lax.broadcasted_iota(jnp.int32, (HALF, HALF * TIMES), 1)
    short = lax.broadcasted_iota(jnp.int32, (HALF, HALF * TIMES), 0)
    chosen = jnp.where(lax.shift_right_logical(long, 3) == short, 1.0, 0.0).astype(jnp.bfloat16)
    for copy in small:
        copy.wait()
    low = low_lanes(4)

    def block(ref, index, lead):
        start = pl.multiple_of(lax.shift_right_logical(index, 1) * 128, 128)
        return own_half(ref[lead + (slice(None), pl.ds(start, 128))], lax.rem(index, 2) == 1)

    def wide_gains(index):
        parts = []
        for part in range(2):
            mine = block(init, index, (part,))
            parts.append(jnp.where(low, mine[:4], swap(mine)[4:]))
        return jnp.concatenate(parts, axis=0)

    mine = pack_all(wide_gains(row))
    chosen_row = mine[0]
    for which in range(1, 8):
        chosen_row = jnp.where(col == which, mine[which], chosen_row)
    previous[...] = chosen_row
    row_flag = block(flags, row, ()).astype(F32)
    row_flag = jnp.where(low_lanes(1), row_flag, swap(row_flag))
    col_flag = jnp.broadcast_to(block(flags, col, ()).astype(F32), (8, 128)).T[:HALF, 0:1]
    col_ids = col * HALF + lax.broadcasted_iota(jnp.int32, (HALF, 128), 0)
    row_ids = row * HALF + (lax.broadcasted_iota(jnp.int32, (HALF, 128), 1) & (HALF - 1))
    scale = jnp.where(col_ids != row_ids, col_flag * row_flag, 0.0)

    dims = (((1,), (1,)), ((), ()))

    def split(j, piece):
        half, at, lanes = piece // 8, piece // 2 % 4 * 16, pl.ds(piece % 2 * 256, 256)
        rows = pl.ds(half * HALF + at, 16)
        vis_re, vis_im = [vis[j, part, half, pl.ds(at, 16), lanes].astype(F32) for part in range(2)]
        mod_re, mod_im = [sky[j, part, half, pl.ds(at, 16), lanes].astype(F32) for part in range(2)]
        values = (
            vis_re * mod_re + vis_im * mod_im,
            vis_im * mod_re - vis_re * mod_im,
            mod_re * mod_re + mod_im * mod_im,
        )
        for which, value in enumerate(values):
            high = value.astype(jnp.bfloat16)
            parts[j % 2, 2 * which, rows, lanes] = high
            parts[j % 2, 2 * which + 1, rows, lanes] = (value - high.astype(F32)).astype(jnp.bfloat16)

    def time_total(j, which):
        high = lax.dot_general(chosen, parts[j % 2, 2 * which], dims, preferred_element_type=F32)
        rest = lax.dot_general(chosen, parts[j % 2, 2 * which + 1], dims, preferred_element_type=F32)
        value = (high + rest) * scale
        for peer in range(PEERS):
            at = (which * 4 + j) * 8
            message[peer, at : at + 8] = value[peer * 8 : peer * 8 + 8]
        return value

    columns = beside(wide_gains(col))
    for line in range(8):
        gain[line] = pick(columns, line)
    for step in range(5):
        totals = []
        if step < 2:
            for copy in (wide[0] if step == 0 else sum(wide[1:], [])):
                copy.wait()
        for piece in range(16):
            if step < 4:
                split(step, piece)
            if step > 0 and piece in (3, 8, 13):
                totals.append(time_total(step - 1, len(totals)))
        if step > 0:
            j = step - 1
            rows = products(*totals, gain[j], gain[4 + j])
            for part in range(3):
                sums[part * 4 + j : part * 4 + j + 1, :] = rows[part]
    share_sums(sums[...], message, TILE_ROWS)


def update_kernel(start, received, previous, message):
    summed = jnp.sum(received[:, start : start + 2], axis=0)
    updated = 0.5 * (summed[0:1] / (summed[1:2] + 1.0) + previous[...])
    message[...] = jnp.broadcast_to(updated, message.shape)


def iterate_kernel(updated, tile, message, previous, gains_of, sums):
    gains = smoothed(updated, lax.axis_index("sub"))
    gains_of[...] = gains
    previous[...] = gains_of[pl.ds(lax.axis_index("row"), 1), :]
    contract(tile, gains, sums)
    share_sums(sums[...], message, 0)


def last_iterate_kernel(updated, tile, message, gains_of, sums):
    gains = smoothed(updated, lax.axis_index("sub"))
    gains_of[...] = gains
    own = gains_of[pl.ds(lax.axis_index("row"), 1), :]
    contract(tile, gains, sums)
    for peer in range(PEERS):
        message[peer, 0:12] = sums[0:12, :]
        message[peer, 12:13] = own


def last_update_kernel(received, message):
    summed = jnp.sum(received[:, 0:12], axis=0)
    previous = jnp.concatenate([received[peer, 12:13] for peer in range(PEERS)], axis=0)
    quotient = summed[0:8] / (twice(summed[8:12]) + 1.0)
    updated = 0.5 * (quotient + jnp.concatenate(pack_all(previous), axis=0))
    means = []
    kept = []
    for part in range(2):
        values = updated[part * 4 : part * 4 + 4]
        total = jnp.sum(values, axis=0, keepdims=True)
        total = (total + swap(total)) / 8.0
        means.append(total)
        kept.append(values - 0.5 * total)
    rest = jnp.concatenate(kept, axis=0)
    mean = jnp.where(low_lanes(1), means[0], means[1])
    for peer in range(PEERS):
        message[peer, 0:8] = rest
        message[peer, 8:9] = mean


def share_kernel(received, message):
    means = jnp.concatenate([received[block, 8:9] for block in range(PEERS)], axis=0)
    for peer in range(PEERS):
        message[peer] = means


def collect_kernel(means, received, out):
    low = low_lanes(4)
    overall = jnp.sum(means[...], axis=0) / 16.0
    other = swap(overall)
    wide = low_lanes(8)
    added = (jnp.where(wide, overall, other), jnp.where(wide, other, overall))
    for part in range(2):
        blocks = [
            received[block, part * 4 : part * 4 + 4] + added[part][block : block + 1] for block in range(PEERS)
        ]
        for pair in range(4):
            even, odd = blocks[2 * pair], blocks[2 * pair + 1]
            out[part, 0:4, pair * 128 : pair * 128 + 128] = jnp.where(low, even, swap(odd))
            out[part, 4:8, pair * 128 : pair * 128 + 128] = jnp.where(low, swap(even), odd)


def shaped(*shape):
    return jax.ShapeDtypeStruct(shape, F32)


def call(name, kernel, outs, *args, scratch=()):
    return pl.pallas_call(
        kernel,
        out_shape=outs,
        in_specs=[VMEM] * len(args),
        out_specs=jax.tree.map(lambda _: VMEM, outs),
        scratch_shapes=scratch,
        compiler_params=pltpu.CompilerParams(vmem_limit_bytes=4 << 20),
        name=name,
    )(*args)


def exchange(message, axis):
    return lax.all_to_all(message, axis, 0, 0, tiled=True)


def body(visibility, sky_model, antenna_flags, gains_init):
    wide = (2, 2, 4, HALF, HALF * TIMES)
    stay = pl.BlockSpec(memory_space=pl.ANY)
    message, previous = pl.pallas_call(
        first_kernel,
        out_shape=(shaped(PEERS, TILE_ROWS + 2, 128), shaped(1, 128)),
        in_specs=[stay] * 4,
        out_specs=(VMEM, VMEM),
        scratch_shapes=[
            pltpu.VMEM((4, 2, 2, HALF, HALF * TIMES), jnp.bfloat16),
            pltpu.VMEM((4, 2, 2, HALF, HALF * TIMES), jnp.bfloat16),
            pltpu.VMEM((1, 512), jnp.int32),
            pltpu.VMEM((2, 8, 512), F32),
            pltpu.VMEM((2, 6, 128, HALF * TIMES), jnp.bfloat16),
            pltpu.VMEM((8, HALF, 128), F32),
            pltpu.VMEM((16, 128), F32),
            pltpu.SemaphoreType.DMA((2,)),
            pltpu.SemaphoreType.DMA((2, 4)),
        ],
        compiler_params=pltpu.CompilerParams(vmem_limit_bytes=FIRST_LIMIT),
        name="first_kernel",
    )(
        *[
            pltpu.with_memory_space_constraint(value, pltpu.HBM)
            for value in (visibility.reshape(wide), sky_model.reshape(wide), antenna_flags, gains_init)
        ]
    )
    tile = received = exchange(message, "col")
    scratch = [pltpu.VMEM((8, 128), F32), pltpu.VMEM((16, 128), F32)]
    for step in range(2):
        kernel = functools.partial(update_kernel, 0 if step else TILE_ROWS)
        message = call("update_kernel", kernel, shaped(PEERS * PEERS, 128), received, previous)
        updated = exchange(message, ("sub", "row")).reshape(PEERS, PEERS, 128)
        if step == 0:
            outs = (shaped(PEERS, 2, 128), shaped(1, 128))
            message, previous = call("iterate_kernel", iterate_kernel, outs, updated, tile, scratch=scratch)
        else:
            outs = shaped(PEERS, 13, 128)
            message = call("last_iterate_kernel", last_iterate_kernel, outs, updated, tile, scratch=scratch)
        received = exchange(message, "col")
    message = call("last_update_kernel", last_update_kernel, shaped(PEERS, 9, 128), received)
    received = exchange(message, "row")
    means = exchange(call("share_kernel", share_kernel, shaped(PEERS, 8, 128), received), "sub")
    return call("collect_kernel", collect_kernel, shaped(2, 8, 512), means, received)


def solution(mesh):
    return jax.shard_map(
        body,
        mesh=mesh,
        in_specs=(
            P(None, "sub", "row", "col"),
            P(None, "sub", "row", "col"),
            P("sub", None),
            P(None, "sub", None),
        ),
        out_specs=P(None, "sub", None),
        check_vma=False,
    )
```

```python
import functools

import jax
import jax.numpy as jnp
from jax import lax
from jax.experimental import pallas as pl
from jax.experimental.pallas import tpu as pltpu
from jax.sharding import PartitionSpec as P


TIMES = 8
PEERS = 8
HALF = 64
F32 = jnp.float32
FIRST_LIMIT = 16 << 20
TILE_ROWS = 96
VMEM = pl.BlockSpec(memory_space=pltpu.VMEM)


def low_lanes(rows):
    return lax.broadcasted_iota(jnp.int32, (rows, 128), 1) < HALF


def swap(value):
    return pltpu.roll(value, HALF, 1)


def own_half(slab, odd):
    return jnp.where(odd, swap(slab), slab)


def pick(turned, low, row, size, which):
    first = jnp.broadcast_to(turned[row : row + size, which : which + 1], (size, 128))
    second = jnp.broadcast_to(turned[row + HALF : row + HALF + size, which : which + 1], (size, 128))
    return jnp.where(low, first, second)


def products(cross_re, cross_im, power, gain_re, gain_im):
    over = lambda value: jnp.sum(value, axis=0, keepdims=True)
    return (
        over(cross_re * gain_re - cross_im * gain_im),
        over(cross_re * gain_im + cross_im * gain_re),
        over(power * (gain_re * gain_re + gain_im * gain_im)),
    )


def lanes_of(rows):
    return lax.broadcasted_iota(jnp.int32, (rows, 128), 1)


def slide(value, step):
    line = lax.broadcasted_iota(jnp.int32, (8, 128), 0)
    out = value
    for row in range(1, 8):
        out = jnp.where(line == row, pltpu.roll(value, (step * row) % 128, 1), out)
    return out


def group_of(rows):
    return lax.shift_right_logical(lanes_of(rows) & (HALF - 1), 3)


def pack_all(wide):
    own = group_of(8) == lax.broadcasted_iota(jnp.int32, (8, 128), 0)
    moved = slide(wide, 8)
    rows = []
    for which in range(8):
        value = jnp.where(own, pltpu.roll(moved, (128 - 8 * which) % 128, 1), 0.0)
        rows.append(jnp.sum(value, axis=0, keepdims=True))
    return rows


def channel_mean(packed):
    lane = lanes_of(8) & 31
    total = packed
    for step in (8, 16, 24):
        total = total + jnp.where(lane >= step, pltpu.roll(packed, step, 1), pltpu.roll(packed, step + 96, 1))
    return (total + swap(total)) / 8.0


def smoothed(updated, sub):
    overall = jnp.sum(updated[...], axis=0) / 8.0
    own = updated[sub]
    return own + 0.5 * channel_mean(overall - own)


def contract(tile, gains, sums):
    turned = gains.T
    low = low_lanes(8)
    totals = [[None] * 3 for _ in range(4)]
    for which in range(8):
        gain = [pick(turned, low, row * 8, 8, which) for row in range(8)]
        for j in range(4):
            cross_re, cross_im, power = [
                tile[which, (part * 4 + j) * 8 : (part * 4 + j) * 8 + 8] for part in range(3)
            ]
            re, im = gain[j], gain[4 + j]
            terms = (cross_re * re - cross_im * im, cross_re * im + cross_im * re, power * (re * re + im * im))
            totals[j] = [term if which == 0 else total + term for total, term in zip(totals[j], terms)]
    for j in range(4):
        for part in range(3):
            sums[part * 4 + j : part * 4 + j + 1, :] = jnp.sum(totals[j][part], axis=0, keepdims=True)


def twice(rows):
    return jnp.concatenate([rows, rows], axis=0)


def share_sums(summed, message, start):
    numerators = pack_all(summed[0:8])
    denominators = pack_all(twice(summed[8:12]))
    for peer in range(PEERS):
        message[peer, start : start + 1] = numerators[peer]
        message[peer, start + 1 : start + 2] = denominators[peer]


def first_kernel(vis_hbm, sky_hbm, flags_hbm, init_hbm, message, previous, vis, sky, flags, init, parts, gain, sums, small_sems, wide_sems):
    row = lax.axis_index("row")
    col = lax.axis_index("col")
    small = [
        pltpu.make_async_copy(flags_hbm, flags, small_sems.at[0]),
        pltpu.make_async_copy(init_hbm, init, small_sems.at[1]),
    ]
    wide = [
        [
            pltpu.make_async_copy(source.at[:, :, j], target.at[j], wide_sems.at[which, j])
            for which, (source, target) in enumerate(((vis_hbm, vis), (sky_hbm, sky)))
        ]
        for j in range(4)
    ]
    for copy in small + sum(wide, []):
        copy.start()

    long = lax.broadcasted_iota(jnp.int32, (HALF, HALF * TIMES), 1)
    short = lax.broadcasted_iota(jnp.int32, (HALF, HALF * TIMES), 0)
    chosen = jnp.where(lax.shift_right_logical(long, 3) == short, 1.0, 0.0).astype(jnp.bfloat16)
    for copy in small:
        copy.wait()
    low = low_lanes(4)

    def block(ref, index, lead):
        start = pl.multiple_of(lax.shift_right_logical(index, 1) * 128, 128)
        return own_half(ref[lead + (slice(None), pl.ds(start, 128))], lax.rem(index, 2) == 1)

    def wide_gains(index):
        parts = []
        for part in range(2):
            mine = block(init, index, (part,))
            parts.append(jnp.where(low, mine[:4], swap(mine)[4:]))
        return jnp.concatenate(parts, axis=0)

    mine = pack_all(wide_gains(row))
    chosen_row = mine[0]
    for which in range(1, 8):
        chosen_row = jnp.where(col == which, mine[which], chosen_row)
    previous[...] = chosen_row
    row_flag = block(flags, row, ()).astype(F32)
    row_flag = jnp.where(low_lanes(1), row_flag, swap(row_flag))
    col_flag = jnp.broadcast_to(block(flags, col, ()).astype(F32), (8, 128)).T[:HALF, 0:1]
    col_ids = col * HALF + lax.broadcasted_iota(jnp.int32, (HALF, 128), 0)
    row_ids = row * HALF + (lax.broadcasted_iota(jnp.int32, (HALF, 128), 1) & (HALF - 1))
    scale = jnp.where(col_ids != row_ids, col_flag * row_flag, 0.0)

    dims = (((1,), (1,)), ((), ()))

    def split(j, piece):
        half, at, lanes = piece // 8, piece // 2 % 4 * 16, pl.ds(piece % 2 * 256, 256)
        rows = pl.ds(half * HALF + at, 16)
        vis_re, vis_im = [vis[j, part, half, pl.ds(at, 16), lanes].astype(F32) for part in range(2)]
        mod_re, mod_im = [sky[j, part, half, pl.ds(at, 16), lanes].astype(F32) for part in range(2)]
        values = (
            vis_re * mod_re + vis_im * mod_im,
            vis_im * mod_re - vis_re * mod_im,
            mod_re * mod_re + mod_im * mod_im,
        )
        for which, value in enumerate(values):
            high = value.astype(jnp.bfloat16)
            parts[j % 2, 2 * which, rows, lanes] = high
            parts[j % 2, 2 * which + 1, rows, lanes] = (value - high.astype(F32)).astype(jnp.bfloat16)

    def time_total(j, which):
        high = lax.dot_general(chosen, parts[j % 2, 2 * which], dims, preferred_element_type=F32)
        rest = lax.dot_general(chosen, parts[j % 2, 2 * which + 1], dims, preferred_element_type=F32)
        value = (high + rest) * scale
        for peer in range(PEERS):
            at = (which * 4 + j) * 8
            message[peer, at : at + 8] = value[peer * 8 : peer * 8 + 8]
        return value

    turned = wide_gains(col).T
    for line in range(8):
        gain[line] = pick(turned, low_lanes(HALF), 0, HALF, line)
    for step in range(5):
        totals = []
        if step < 2:
            for copy in (wide[0] if step == 0 else sum(wide[1:], [])):
                copy.wait()
        for piece in range(16):
            if step < 4:
                split(step, piece)
            if step > 0 and piece in (3, 8, 13):
                totals.append(time_total(step - 1, len(totals)))
        if step > 0:
            j = step - 1
            rows = products(*totals, gain[j], gain[4 + j])
            for part in range(3):
                sums[part * 4 + j : part * 4 + j + 1, :] = rows[part]
    share_sums(sums[...], message, TILE_ROWS)


def update_kernel(start, received, previous, message):
    summed = jnp.sum(received[:, start : start + 2], axis=0)
    updated = 0.5 * (summed[0:1] / (summed[1:2] + 1.0) + previous[...])
    message[...] = jnp.broadcast_to(updated, message.shape)


def iterate_kernel(updated, tile, message, previous, gains_of, sums):
    gains = smoothed(updated, lax.axis_index("sub"))
    gains_of[...] = gains
    previous[...] = gains_of[pl.ds(lax.axis_index("row"), 1), :]
    contract(tile, gains, sums)
    share_sums(sums[...], message, 0)


def last_iterate_kernel(updated, tile, message, gains_of, sums):
    gains = smoothed(updated, lax.axis_index("sub"))
    gains_of[...] = gains
    own = gains_of[pl.ds(lax.axis_index("row"), 1), :]
    contract(tile, gains, sums)
    for peer in range(PEERS):
        message[peer, 0:12] = sums[0:12, :]
        message[peer, 12:13] = own


def last_update_kernel(received, message):
    summed = jnp.sum(received[:, 0:12], axis=0)
    previous = jnp.concatenate([received[peer, 12:13] for peer in range(PEERS)], axis=0)
    quotient = summed[0:8] / (twice(summed[8:12]) + 1.0)
    updated = 0.5 * (quotient + jnp.concatenate(pack_all(previous), axis=0))
    means = []
    kept = []
    for part in range(2):
        values = updated[part * 4 : part * 4 + 4]
        total = jnp.sum(values, axis=0, keepdims=True)
        total = (total + swap(total)) / 8.0
        means.append(total)
        kept.append(values - 0.5 * total)
    rest = jnp.concatenate(kept, axis=0)
    mean = jnp.where(low_lanes(1), means[0], means[1])
    for peer in range(PEERS):
        message[peer, 0:8] = rest
        message[peer, 8:9] = mean


def share_kernel(received, message):
    means = jnp.concatenate([received[block, 8:9] for block in range(PEERS)], axis=0)
    for peer in range(PEERS):
        message[peer] = means


def collect_kernel(means, received, out):
    low = low_lanes(4)
    overall = jnp.sum(means[...], axis=0) / 16.0
    other = swap(overall)
    wide = low_lanes(8)
    added = (jnp.where(wide, overall, other), jnp.where(wide, other, overall))
    for part in range(2):
        blocks = [
            received[block, part * 4 : part * 4 + 4] + added[part][block : block + 1] for block in range(PEERS)
        ]
        for pair in range(4):
            even, odd = blocks[2 * pair], blocks[2 * pair + 1]
            out[part, 0:4, pair * 128 : pair * 128 + 128] = jnp.where(low, even, swap(odd))
            out[part, 4:8, pair * 128 : pair * 128 + 128] = jnp.where(low, swap(even), odd)


def shaped(*shape):
    return jax.ShapeDtypeStruct(shape, F32)


def call(name, kernel, outs, *args, scratch=()):
    return pl.pallas_call(
        kernel,
        out_shape=outs,
        in_specs=[VMEM] * len(args),
        out_specs=jax.tree.map(lambda _: VMEM, outs),
        scratch_shapes=scratch,
        compiler_params=pltpu.CompilerParams(vmem_limit_bytes=4 << 20),
        name=name,
    )(*args)


def exchange(message, axis):
    return lax.all_to_all(message, axis, 0, 0, tiled=True)


def body(visibility, sky_model, antenna_flags, gains_init):
    wide = (2, 2, 4, HALF, HALF * TIMES)
    stay = pl.BlockSpec(memory_space=pl.ANY)
    message, previous = pl.pallas_call(
        first_kernel,
        out_shape=(shaped(PEERS, TILE_ROWS + 2, 128), shaped(1, 128)),
        in_specs=[stay] * 4,
        out_specs=(VMEM, VMEM),
        scratch_shapes=[
            pltpu.VMEM((4, 2, 2, HALF, HALF * TIMES), jnp.bfloat16),
            pltpu.VMEM((4, 2, 2, HALF, HALF * TIMES), jnp.bfloat16),
            pltpu.VMEM((1, 512), jnp.int32),
            pltpu.VMEM((2, 8, 512), F32),
            pltpu.VMEM((2, 6, 128, HALF * TIMES), jnp.bfloat16),
            pltpu.VMEM((8, HALF, 128), F32),
            pltpu.VMEM((16, 128), F32),
            pltpu.SemaphoreType.DMA((2,)),
            pltpu.SemaphoreType.DMA((2, 4)),
        ],
        compiler_params=pltpu.CompilerParams(vmem_limit_bytes=FIRST_LIMIT),
        name="first_kernel",
    )(
        *[
            pltpu.with_memory_space_constraint(value, pltpu.HBM)
            for value in (visibility.reshape(wide), sky_model.reshape(wide), antenna_flags, gains_init)
        ]
    )
    tile = received = exchange(message, "col")
    scratch = [pltpu.VMEM((8, 128), F32), pltpu.VMEM((16, 128), F32)]
    for step in range(2):
        kernel = functools.partial(update_kernel, 0 if step else TILE_ROWS)
        message = call("update_kernel", kernel, shaped(PEERS * PEERS, 128), received, previous)
        updated = exchange(message, ("sub", "row")).reshape(PEERS, PEERS, 128)
        if step == 0:
            outs = (shaped(PEERS, 2, 128), shaped(1, 128))
            message, previous = call("iterate_kernel", iterate_kernel, outs, updated, tile, scratch=scratch)
        else:
            outs = shaped(PEERS, 13, 128)
            message = call("last_iterate_kernel", last_iterate_kernel, outs, updated, tile, scratch=scratch)
        received = exchange(message, "col")
    message = call("last_update_kernel", last_update_kernel, shaped(PEERS, 9, 128), received)
    received = exchange(message, "row")
    means = exchange(call("share_kernel", share_kernel, shaped(PEERS, 8, 128), received), "sub")
    return call("collect_kernel", collect_kernel, shaped(2, 8, 512), means, received)


def solution(mesh):
    return jax.shard_map(
        body,
        mesh=mesh,
        in_specs=(
            P(None, "sub", "row", "col"),
            P(None, "sub", "row", "col"),
            P("sub", None),
            P(None, "sub", None),
        ),
        out_specs=P(None, "sub", None),
        check_vma=False,
    )
```

```python
import functools

import jax
import jax.numpy as jnp
from jax import lax
from jax.experimental import pallas as pl
from jax.experimental.pallas import tpu as pltpu
from jax.sharding import PartitionSpec as P


TIMES = 8
PEERS = 8
HALF = 64
F32 = jnp.float32
FIRST_LIMIT = 16 << 20
TILE_ROWS = 96
VMEM = pl.BlockSpec(memory_space=pltpu.VMEM)


def low_lanes(rows):
    return lax.broadcasted_iota(jnp.int32, (rows, 128), 1) < HALF


def swap(value):
    return pltpu.roll(value, HALF, 1)


def own_half(slab, odd):
    return jnp.where(odd, swap(slab), slab)


def pick(turned, low, row, size, which):
    first = jnp.broadcast_to(turned[row : row + size, which : which + 1], (size, 128))
    second = jnp.broadcast_to(turned[row + HALF : row + HALF + size, which : which + 1], (size, 128))
    return jnp.where(low, first, second)


def products(cross_re, cross_im, power, gain_re, gain_im):
    over = lambda value: jnp.sum(value, axis=0, keepdims=True)
    return (
        over(cross_re * gain_re - cross_im * gain_im),
        over(cross_re * gain_im + cross_im * gain_re),
        over(power * (gain_re * gain_re + gain_im * gain_im)),
    )


def lanes_of(rows):
    return lax.broadcasted_iota(jnp.int32, (rows, 128), 1)


def slide(value, step):
    line = lax.broadcasted_iota(jnp.int32, (8, 128), 0)
    out = value
    for row in range(1, 8):
        out = jnp.where(line == row, pltpu.roll(value, (step * row) % 128, 1), out)
    return out


def group_of(rows):
    return lax.shift_right_logical(lanes_of(rows) & (HALF - 1), 3)


def pack_all(wide):
    own = group_of(8) == lax.broadcasted_iota(jnp.int32, (8, 128), 0)
    moved = slide(wide, 8)
    rows = []
    for which in range(8):
        value = jnp.where(own, pltpu.roll(moved, (128 - 8 * which) % 128, 1), 0.0)
        rows.append(jnp.sum(value, axis=0, keepdims=True))
    return rows


def channel_mean(packed):
    lane = lanes_of(8) & 31
    total = packed
    for step in (8, 16, 24):
        total = total + jnp.where(lane >= step, pltpu.roll(packed, step, 1), pltpu.roll(packed, step + 96, 1))
    return (total + swap(total)) / 8.0


def smoothed(updated, sub):
    overall = jnp.sum(updated[...], axis=0) / 8.0
    own = updated[sub]
    return own + 0.5 * channel_mean(overall - own)


def contract(tile, gains, sums):
    turned = gains.T
    low = low_lanes(8)
    gain = [[pick(turned, low, row * 8, 8, which) for which in range(8)] for row in range(8)]
    for j in range(4):
        totals = [jnp.zeros((8, 128), F32)] * 3
        for which in range(8):
            cross_re, cross_im, power = [
                tile[which, (part * 4 + j) * 8 : (part * 4 + j) * 8 + 8] for part in range(3)
            ]
            re, im = gain[j][which], gain[4 + j][which]
            totals[0] += cross_re * re - cross_im * im
            totals[1] += cross_re * im + cross_im * re
            totals[2] += power * (re * re + im * im)
        for part in range(3):
            sums[part * 4 + j : part * 4 + j + 1, :] = jnp.sum(totals[part], axis=0, keepdims=True)


def twice(rows):
    return jnp.concatenate([rows, rows], axis=0)


def share_sums(summed, message, start):
    numerators = pack_all(summed[0:8])
    denominators = pack_all(twice(summed[8:12]))
    for peer in range(PEERS):
        message[peer, start : start + 1] = numerators[peer]
        message[peer, start + 1 : start + 2] = denominators[peer]


def first_kernel(vis_hbm, sky_hbm, flags_hbm, init_hbm, message, previous, vis, sky, flags, init, parts, gain, sums, small_sems, wide_sems):
    row = lax.axis_index("row")
    col = lax.axis_index("col")
    small = [
        pltpu.make_async_copy(flags_hbm, flags, small_sems.at[0]),
        pltpu.make_async_copy(init_hbm, init, small_sems.at[1]),
    ]
    wide = [
        [
            pltpu.make_async_copy(source.at[:, :, j], target.at[j], wide_sems.at[which, j])
            for which, (source, target) in enumerate(((vis_hbm, vis), (sky_hbm, sky)))
        ]
        for j in range(4)
    ]
    for copy in small + sum(wide, []):
        copy.start()

    long = lax.broadcasted_iota(jnp.int32, (HALF, HALF * TIMES), 1)
    short = lax.broadcasted_iota(jnp.int32, (HALF, HALF * TIMES), 0)
    chosen = jnp.where(lax.shift_right_logical(long, 3) == short, 1.0, 0.0).astype(jnp.bfloat16)
    for copy in small:
        copy.wait()
    low = low_lanes(4)

    def block(ref, index, lead):
        start = pl.multiple_of(lax.shift_right_logical(index, 1) * 128, 128)
        return own_half(ref[lead + (slice(None), pl.ds(start, 128))], lax.rem(index, 2) == 1)

    def wide_gains(index):
        parts = []
        for part in range(2):
            mine = block(init, index, (part,))
            parts.append(jnp.where(low, mine[:4], swap(mine)[4:]))
        return jnp.concatenate(parts, axis=0)

    mine = pack_all(wide_gains(row))
    chosen_row = mine[0]
    for which in range(1, 8):
        chosen_row = jnp.where(col == which, mine[which], chosen_row)
    previous[...] = chosen_row
    row_flag = block(flags, row, ()).astype(F32)
    row_flag = jnp.where(low_lanes(1), row_flag, swap(row_flag))
    col_flag = jnp.broadcast_to(block(flags, col, ()).astype(F32), (8, 128)).T[:HALF, 0:1]
    col_ids = col * HALF + lax.broadcasted_iota(jnp.int32, (HALF, 128), 0)
    row_ids = row * HALF + (lax.broadcasted_iota(jnp.int32, (HALF, 128), 1) & (HALF - 1))
    scale = jnp.where(col_ids != row_ids, col_flag * row_flag, 0.0)

    dims = (((1,), (1,)), ((), ()))

    def split(j, piece):
        half, at, lanes = piece // 8, piece // 2 % 4 * 16, pl.ds(piece % 2 * 256, 256)
        rows = pl.ds(half * HALF + at, 16)
        vis_re, vis_im = [vis[j, part, half, pl.ds(at, 16), lanes].astype(F32) for part in range(2)]
        mod_re, mod_im = [sky[j, part, half, pl.ds(at, 16), lanes].astype(F32) for part in range(2)]
        values = (
            vis_re * mod_re + vis_im * mod_im,
            vis_im * mod_re - vis_re * mod_im,
            mod_re * mod_re + mod_im * mod_im,
        )
        for which, value in enumerate(values):
            high = value.astype(jnp.bfloat16)
            parts[j % 2, 2 * which, rows, lanes] = high
            parts[j % 2, 2 * which + 1, rows, lanes] = (value - high.astype(F32)).astype(jnp.bfloat16)

    def time_total(j, which):
        high = lax.dot_general(chosen, parts[j % 2, 2 * which], dims, preferred_element_type=F32)
        rest = lax.dot_general(chosen, parts[j % 2, 2 * which + 1], dims, preferred_element_type=F32)
        value = (high + rest) * scale
        for peer in range(PEERS):
            at = (which * 4 + j) * 8
            message[peer, at : at + 8] = value[peer * 8 : peer * 8 + 8]
        return value

    turned = wide_gains(col).T
    for line in range(8):
        gain[line] = pick(turned, low_lanes(HALF), 0, HALF, line)
    for step in range(5):
        totals = []
        if step < 2:
            for copy in (wide[0] if step == 0 else sum(wide[1:], [])):
                copy.wait()
        for piece in range(16):
            if step < 4:
                split(step, piece)
            if step > 0 and piece in (3, 8, 13):
                totals.append(time_total(step - 1, len(totals)))
        if step > 0:
            j = step - 1
            rows = products(*totals, gain[j], gain[4 + j])
            for part in range(3):
                sums[part * 4 + j : part * 4 + j + 1, :] = rows[part]
    share_sums(sums[...], message, TILE_ROWS)


def update_kernel(start, received, previous, message):
    summed = jnp.sum(received[:, start : start + 2], axis=0)
    updated = 0.5 * (summed[0:1] / (summed[1:2] + 1.0) + previous[...])
    message[...] = jnp.broadcast_to(updated, message.shape)


def iterate_kernel(updated, tile, message, previous, gains_of, sums):
    gains = smoothed(updated, lax.axis_index("sub"))
    gains_of[...] = gains
    previous[...] = gains_of[pl.ds(lax.axis_index("row"), 1), :]
    contract(tile, gains, sums)
    share_sums(sums[...], message, 0)


def last_iterate_kernel(updated, tile, message, gains_of, sums):
    gains = smoothed(updated, lax.axis_index("sub"))
    gains_of[...] = gains
    own = gains_of[pl.ds(lax.axis_index("row"), 1), :]
    contract(tile, gains, sums)
    for peer in range(PEERS):
        message[peer, 0:12] = sums[0:12, :]
        message[peer, 12:13] = own


def last_update_kernel(received, message):
    summed = jnp.sum(received[:, 0:12], axis=0)
    previous = jnp.concatenate([received[peer, 12:13] for peer in range(PEERS)], axis=0)
    quotient = summed[0:8] / (twice(summed[8:12]) + 1.0)
    updated = 0.5 * (quotient + jnp.concatenate(pack_all(previous), axis=0))
    means = []
    kept = []
    for part in range(2):
        values = updated[part * 4 : part * 4 + 4]
        total = jnp.sum(values, axis=0, keepdims=True)
        total = (total + swap(total)) / 8.0
        means.append(total)
        kept.append(values - 0.5 * total)
    rest = jnp.concatenate(kept, axis=0)
    mean = jnp.where(low_lanes(1), means[0], means[1])
    for peer in range(PEERS):
        message[peer, 0:8] = rest
        message[peer, 8:9] = mean


def share_kernel(received, message):
    means = jnp.concatenate([received[block, 8:9] for block in range(PEERS)], axis=0)
    for peer in range(PEERS):
        message[peer] = means


def collect_kernel(means, received, out):
    low = low_lanes(4)
    overall = jnp.sum(means[...], axis=0) / 16.0
    other = swap(overall)
    wide = low_lanes(8)
    added = (jnp.where(wide, overall, other), jnp.where(wide, other, overall))
    for part in range(2):
        blocks = [
            received[block, part * 4 : part * 4 + 4] + added[part][block : block + 1] for block in range(PEERS)
        ]
        for pair in range(4):
            even, odd = blocks[2 * pair], blocks[2 * pair + 1]
            out[part, 0:4, pair * 128 : pair * 128 + 128] = jnp.where(low, even, swap(odd))
            out[part, 4:8, pair * 128 : pair * 128 + 128] = jnp.where(low, swap(even), odd)


def shaped(*shape):
    return jax.ShapeDtypeStruct(shape, F32)


def call(name, kernel, outs, *args, scratch=()):
    return pl.pallas_call(
        kernel,
        out_shape=outs,
        in_specs=[VMEM] * len(args),
        out_specs=jax.tree.map(lambda _: VMEM, outs),
        scratch_shapes=scratch,
        compiler_params=pltpu.CompilerParams(vmem_limit_bytes=4 << 20),
        name=name,
    )(*args)


def exchange(message, axis):
    return lax.all_to_all(message, axis, 0, 0, tiled=True)


def body(visibility, sky_model, antenna_flags, gains_init):
    wide = (2, 2, 4, HALF, HALF * TIMES)
    stay = pl.BlockSpec(memory_space=pl.ANY)
    message, previous = pl.pallas_call(
        first_kernel,
        out_shape=(shaped(PEERS, TILE_ROWS + 2, 128), shaped(1, 128)),
        in_specs=[stay] * 4,
        out_specs=(VMEM, VMEM),
        scratch_shapes=[
            pltpu.VMEM((4, 2, 2, HALF, HALF * TIMES), jnp.bfloat16),
            pltpu.VMEM((4, 2, 2, HALF, HALF * TIMES), jnp.bfloat16),
            pltpu.VMEM((1, 512), jnp.int32),
            pltpu.VMEM((2, 8, 512), F32),
            pltpu.VMEM((2, 6, 128, HALF * TIMES), jnp.bfloat16),
            pltpu.VMEM((8, HALF, 128), F32),
            pltpu.VMEM((16, 128), F32),
            pltpu.SemaphoreType.DMA((2,)),
            pltpu.SemaphoreType.DMA((2, 4)),
        ],
        compiler_params=pltpu.CompilerParams(vmem_limit_bytes=FIRST_LIMIT),
        name="first_kernel",
    )(
        *[
            pltpu.with_memory_space_constraint(value, pltpu.HBM)
            for value in (visibility.reshape(wide), sky_model.reshape(wide), antenna_flags, gains_init)
        ]
    )
    tile = received = exchange(message, "col")
    scratch = [pltpu.VMEM((8, 128), F32), pltpu.VMEM((16, 128), F32)]
    for step in range(2):
        kernel = functools.partial(update_kernel, 0 if step else TILE_ROWS)
        message = call("update_kernel", kernel, shaped(PEERS * PEERS, 128), received, previous)
        updated = exchange(message, ("sub", "row")).reshape(PEERS, PEERS, 128)
        if step == 0:
            outs = (shaped(PEERS, 2, 128), shaped(1, 128))
            message, previous = call("iterate_kernel", iterate_kernel, outs, updated, tile, scratch=scratch)
        else:
            outs = shaped(PEERS, 13, 128)
            message = call("last_iterate_kernel", last_iterate_kernel, outs, updated, tile, scratch=scratch)
        received = exchange(message, "col")
    message = call("last_update_kernel", last_update_kernel, shaped(PEERS, 9, 128), received)
    received = exchange(message, "row")
    means = exchange(call("share_kernel", share_kernel, shaped(PEERS, 8, 128), received), "sub")
    return call("collect_kernel", collect_kernel, shaped(2, 8, 512), means, received)


def solution(mesh):
    return jax.shard_map(
        body,
        mesh=mesh,
        in_specs=(
            P(None, "sub", "row", "col"),
            P(None, "sub", "row", "col"),
            P("sub", None),
            P(None, "sub", None),
        ),
        out_specs=P(None, "sub", None),
        check_vma=False,
    )
```

```python
import functools

import jax
import jax.numpy as jnp
from jax import lax
from jax.experimental import pallas as pl
from jax.experimental.pallas import tpu as pltpu
from jax.sharding import PartitionSpec as P


TIMES = 8
PEERS = 8
HALF = 64
F32 = jnp.float32
FIRST_LIMIT = 16 << 20
TILE_ROWS = 96
VMEM = pl.BlockSpec(memory_space=pltpu.VMEM)


def low_lanes(rows):
    return lax.broadcasted_iota(jnp.int32, (rows, 128), 1) < HALF


def swap(value):
    return pltpu.roll(value, HALF, 1)


def own_half(slab, odd):
    return jnp.where(odd, swap(slab), slab)


def pick(turned, low, row, size, which):
    first = jnp.broadcast_to(turned[row : row + size, which : which + 1], (size, 128))
    second = jnp.broadcast_to(turned[row + HALF : row + HALF + size, which : which + 1], (size, 128))
    return jnp.where(low, first, second)


def products(cross_re, cross_im, power, gain_re, gain_im):
    over = lambda value: jnp.sum(value, axis=0, keepdims=True)
    return (
        over(cross_re * gain_re - cross_im * gain_im),
        over(cross_re * gain_im + cross_im * gain_re),
        over(power * (gain_re * gain_re + gain_im * gain_im)),
    )


def lanes_of(rows):
    return lax.broadcasted_iota(jnp.int32, (rows, 128), 1)


def slide(value, step):
    line = lax.broadcasted_iota(jnp.int32, (8, 128), 0)
    out = value
    for row in range(1, 8):
        out = jnp.where(line == row, pltpu.roll(value, (step * row) % 128, 1), out)
    return out


def group_of(rows):
    return lax.shift_right_logical(lanes_of(rows) & (HALF - 1), 3)


def pack_all(wide):
    own = group_of(8) == lax.broadcasted_iota(jnp.int32, (8, 128), 0)
    moved = slide(wide, 8)
    rows = []
    for which in range(8):
        value = jnp.where(own, pltpu.roll(moved, (128 - 8 * which) % 128, 1), 0.0)
        rows.append(jnp.sum(value, axis=0, keepdims=True))
    return rows


def channel_mean(packed):
    lane = lanes_of(8) & 31
    total = packed
    for step in (8, 16, 24):
        total = total + jnp.where(lane >= step, pltpu.roll(packed, step, 1), pltpu.roll(packed, step + 96, 1))
    return (total + swap(total)) / 8.0


def smoothed(updated, sub):
    overall = jnp.sum(updated[...], axis=0) / 8.0
    own = updated[sub]
    return own + 0.5 * channel_mean(overall - own)


def contract(tile, gains, sums):
    turned = gains.T
    low = low_lanes(8)
    totals = [[None] * 3 for _ in range(4)]
    for which in range(8):
        gain = [pick(turned, low, row * 8, 8, which) for row in range(8)]
        for j in range(4):
            cross_re, cross_im, power = [
                tile[which, (part * 4 + j) * 8 : (part * 4 + j) * 8 + 8] for part in range(3)
            ]
            re, im = gain[j], gain[4 + j]
            terms = (cross_re * re - cross_im * im, cross_re * im + cross_im * re, power * (re * re + im * im))
            totals[j] = [term if which == 0 else total + term for total, term in zip(totals[j], terms)]
    for j in range(4):
        for part in range(3):
            sums[part * 4 + j : part * 4 + j + 1, :] = jnp.sum(totals[j][part], axis=0, keepdims=True)


def twice(rows):
    return jnp.concatenate([rows, rows], axis=0)


def share_sums(summed, message, start):
    numerators = pack_all(summed[0:8])
    denominators = pack_all(twice(summed[8:12]))
    for peer in range(PEERS):
        message[peer, start : start + 1] = numerators[peer]
        message[peer, start + 1 : start + 2] = denominators[peer]


def first_kernel(vis_hbm, sky_hbm, flags_hbm, init_hbm, message, previous, vis, sky, flags, init, parts, gain, sums, small_sems, wide_sems):
    row = lax.axis_index("row")
    col = lax.axis_index("col")
    small = [
        pltpu.make_async_copy(flags_hbm, flags, small_sems.at[0]),
        pltpu.make_async_copy(init_hbm, init, small_sems.at[1]),
    ]
    wide = [
        [
            pltpu.make_async_copy(source.at[:, :, j], target.at[j], wide_sems.at[which, j])
            for which, (source, target) in enumerate(((vis_hbm, vis), (sky_hbm, sky)))
        ]
        for j in range(4)
    ]
    for copy in small + sum(wide, []):
        copy.start()

    long = lax.broadcasted_iota(jnp.int32, (HALF, HALF * TIMES), 1)
    short = lax.broadcasted_iota(jnp.int32, (HALF, HALF * TIMES), 0)
    chosen = jnp.where(lax.shift_right_logical(long, 3) == short, 1.0, 0.0).astype(jnp.bfloat16)
    for copy in small:
        copy.wait()
    low = low_lanes(4)

    def block(ref, index, lead):
        start = pl.multiple_of(lax.shift_right_logical(index, 1) * 128, 128)
        return own_half(ref[lead + (slice(None), pl.ds(start, 128))], lax.rem(index, 2) == 1)

    def wide_gains(index):
        parts = []
        for part in range(2):
            mine = block(init, index, (part,))
            parts.append(jnp.where(low, mine[:4], swap(mine)[4:]))
        return jnp.concatenate(parts, axis=0)

    mine = pack_all(wide_gains(row))
    chosen_row = mine[0]
    for which in range(1, 8):
        chosen_row = jnp.where(col == which, mine[which], chosen_row)
    previous[...] = chosen_row
    row_flag = block(flags, row, ()).astype(F32)
    row_flag = jnp.where(low_lanes(1), row_flag, swap(row_flag))
    col_flag = jnp.broadcast_to(block(flags, col, ()).astype(F32), (8, 128)).T[:HALF, 0:1]
    col_ids = col * HALF + lax.broadcasted_iota(jnp.int32, (HALF, 128), 0)
    row_ids = row * HALF + (lax.broadcasted_iota(jnp.int32, (HALF, 128), 1) & (HALF - 1))
    scale = jnp.where(col_ids != row_ids, col_flag * row_flag, 0.0)

    dims = (((1,), (1,)), ((), ()))

    def split(j, piece):
        half, at, lanes = piece // 8, piece // 2 % 4 * 16, pl.ds(piece % 2 * 256, 256)
        rows = pl.ds(half * HALF + at, 16)
        vis_re, vis_im = [vis[j, part, half, pl.ds(at, 16), lanes].astype(F32) for part in range(2)]
        mod_re, mod_im = [sky[j, part, half, pl.ds(at, 16), lanes].astype(F32) for part in range(2)]
        values = (
            vis_re * mod_re + vis_im * mod_im,
            vis_im * mod_re - vis_re * mod_im,
            mod_re * mod_re + mod_im * mod_im,
        )
        for which, value in enumerate(values):
            high = value.astype(jnp.bfloat16)
            parts[j % 2, 2 * which, rows, lanes] = high
            parts[j % 2, 2 * which + 1, rows, lanes] = (value - high.astype(F32)).astype(jnp.bfloat16)

    def time_total(j, which):
        high = lax.dot_general(chosen, parts[j % 2, 2 * which], dims, preferred_element_type=F32)
        rest = lax.dot_general(chosen, parts[j % 2, 2 * which + 1], dims, preferred_element_type=F32)
        value = (high + rest) * scale
        for peer in range(PEERS):
            at = (which * 4 + j) * 8
            message[peer, at : at + 8] = value[peer * 8 : peer * 8 + 8]
        return value

    turned = wide_gains(col).T
    for line in range(8):
        gain[line] = pick(turned, low_lanes(HALF), 0, HALF, line)
    for step in range(5):
        totals = []
        if step == 0:
            for copy in sum(wide, []):
                copy.wait()
        for piece in range(16):
            if step < 4:
                split(step, piece)
            if step > 0 and piece in (3, 8, 13):
                totals.append(time_total(step - 1, len(totals)))
        if step > 0:
            j = step - 1
            rows = products(*totals, gain[j], gain[4 + j])
            for part in range(3):
                sums[part * 4 + j : part * 4 + j + 1, :] = rows[part]
    share_sums(sums[...], message, TILE_ROWS)


def update_kernel(start, received, previous, message):
    summed = jnp.sum(received[:, start : start + 2], axis=0)
    updated = 0.5 * (summed[0:1] / (summed[1:2] + 1.0) + previous[...])
    message[...] = jnp.broadcast_to(updated, message.shape)


def iterate_kernel(updated, tile, message, previous, gains_of, sums):
    gains = smoothed(updated, lax.axis_index("sub"))
    gains_of[...] = gains
    previous[...] = gains_of[pl.ds(lax.axis_index("row"), 1), :]
    contract(tile, gains, sums)
    share_sums(sums[...], message, 0)


def last_iterate_kernel(updated, tile, message, gains_of, sums):
    gains = smoothed(updated, lax.axis_index("sub"))
    gains_of[...] = gains
    own = gains_of[pl.ds(lax.axis_index("row"), 1), :]
    contract(tile, gains, sums)
    for peer in range(PEERS):
        message[peer, 0:12] = sums[0:12, :]
        message[peer, 12:13] = own


def last_update_kernel(received, message):
    summed = jnp.sum(received[:, 0:12], axis=0)
    previous = jnp.concatenate([received[peer, 12:13] for peer in range(PEERS)], axis=0)
    quotient = summed[0:8] / (twice(summed[8:12]) + 1.0)
    updated = 0.5 * (quotient + jnp.concatenate(pack_all(previous), axis=0))
    means = []
    kept = []
    for part in range(2):
        values = updated[part * 4 : part * 4 + 4]
        total = jnp.sum(values, axis=0, keepdims=True)
        total = (total + swap(total)) / 8.0
        means.append(total)
        kept.append(values - 0.5 * total)
    rest = jnp.concatenate(kept, axis=0)
    mean = jnp.where(low_lanes(1), means[0], means[1])
    for peer in range(PEERS):
        message[peer, 0:8] = rest
        message[peer, 8:9] = mean


def share_kernel(received, message):
    means = jnp.concatenate([received[block, 8:9] for block in range(PEERS)], axis=0)
    for peer in range(PEERS):
        message[peer] = means


def collect_kernel(means, received, out):
    low = low_lanes(4)
    overall = jnp.sum(means[...], axis=0) / 16.0
    other = swap(overall)
    wide = low_lanes(8)
    added = (jnp.where(wide, overall, other), jnp.where(wide, other, overall))
    for part in range(2):
        blocks = [
            received[block, part * 4 : part * 4 + 4] + added[part][block : block + 1] for block in range(PEERS)
        ]
        for pair in range(4):
            even, odd = blocks[2 * pair], blocks[2 * pair + 1]
            out[part, 0:4, pair * 128 : pair * 128 + 128] = jnp.where(low, even, swap(odd))
            out[part, 4:8, pair * 128 : pair * 128 + 128] = jnp.where(low, swap(even), odd)


def shaped(*shape):
    return jax.ShapeDtypeStruct(shape, F32)


def call(name, kernel, outs, *args, scratch=()):
    return pl.pallas_call(
        kernel,
        out_shape=outs,
        in_specs=[VMEM] * len(args),
        out_specs=jax.tree.map(lambda _: VMEM, outs),
        scratch_shapes=scratch,
        compiler_params=pltpu.CompilerParams(vmem_limit_bytes=4 << 20),
        name=name,
    )(*args)


def exchange(message, axis):
    return lax.all_to_all(message, axis, 0, 0, tiled=True)


def body(visibility, sky_model, antenna_flags, gains_init):
    wide = (2, 2, 4, HALF, HALF * TIMES)
    stay = pl.BlockSpec(memory_space=pl.ANY)
    message, previous = pl.pallas_call(
        first_kernel,
        out_shape=(shaped(PEERS, TILE_ROWS + 2, 128), shaped(1, 128)),
        in_specs=[stay] * 4,
        out_specs=(VMEM, VMEM),
        scratch_shapes=[
            pltpu.VMEM((4, 2, 2, HALF, HALF * TIMES), jnp.bfloat16),
            pltpu.VMEM((4, 2, 2, HALF, HALF * TIMES), jnp.bfloat16),
            pltpu.VMEM((1, 512), jnp.int32),
            pltpu.VMEM((2, 8, 512), F32),
            pltpu.VMEM((2, 6, 128, HALF * TIMES), jnp.bfloat16),
            pltpu.VMEM((8, HALF, 128), F32),
            pltpu.VMEM((16, 128), F32),
            pltpu.SemaphoreType.DMA((2,)),
            pltpu.SemaphoreType.DMA((2, 4)),
        ],
        compiler_params=pltpu.CompilerParams(vmem_limit_bytes=FIRST_LIMIT),
        name="first_kernel",
    )(
        *[
            pltpu.with_memory_space_constraint(value, pltpu.HBM)
            for value in (visibility.reshape(wide), sky_model.reshape(wide), antenna_flags, gains_init)
        ]
    )
    tile = received = exchange(message, "col")
    scratch = [pltpu.VMEM((8, 128), F32), pltpu.VMEM((16, 128), F32)]
    for step in range(2):
        kernel = functools.partial(update_kernel, 0 if step else TILE_ROWS)
        message = call("update_kernel", kernel, shaped(PEERS * PEERS, 128), received, previous)
        updated = exchange(message, ("sub", "row")).reshape(PEERS, PEERS, 128)
        if step == 0:
            outs = (shaped(PEERS, 2, 128), shaped(1, 128))
            message, previous = call("iterate_kernel", iterate_kernel, outs, updated, tile, scratch=scratch)
        else:
            outs = shaped(PEERS, 13, 128)
            message = call("last_iterate_kernel", last_iterate_kernel, outs, updated, tile, scratch=scratch)
        received = exchange(message, "col")
    message = call("last_update_kernel", last_update_kernel, shaped(PEERS, 9, 128), received)
    received = exchange(message, "row")
    means = exchange(call("share_kernel", share_kernel, shaped(PEERS, 8, 128), received), "sub")
    return call("collect_kernel", collect_kernel, shaped(2, 8, 512), means, received)


def solution(mesh):
    return jax.shard_map(
        body,
        mesh=mesh,
        in_specs=(
            P(None, "sub", "row", "col"),
            P(None, "sub", "row", "col"),
            P("sub", None),
            P(None, "sub", None),
        ),
        out_specs=P(None, "sub", None),
        check_vma=False,
    )
```
